256 devices in a mesh: top: 4 (over x_lo, core), mid: 2 (over x_hi), leaf: 32 (over y, z).
Axes of the slice: x: 4 (x_hi: 2, x_lo: 2; x = x_hi * 2 + x_lo), y: 4, z: 8, core: 2. Of those that a mesh axis runs over, the one named last changes fastest.
Arguments:
- rhs: bfloat16 [393216, 256], P(('top', 'mid', 'leaf')), may hold values from -6 to 6
- guess: bfloat16 [393216, 256], P(('top', 'mid', 'leaf')), may hold values from -3 to 3
- diag_blocks: bfloat16 [256, 1536, 1536], P(('top', 'mid', 'leaf')), as said below
- precond: bfloat16 [256, 1536, 1536], P(('top', 'mid', 'leaf'))
- bases: bfloat16 [256, 1536, 128], P(('top', 'mid', 'leaf')), may hold values from -0.3125 to 0.3125
- leaf_to_middle_transfer: bfloat16 [256, 128, 128], P(('top', 'mid', 'leaf')), may hold values from -0.25 to 0.25
- mid_transfer: bfloat16 [8, 128, 128], replicated, may hold values from -0.375 to 0.375
- leaf_coupling: bfloat16 [256, 4, 128, 128], P(('top', 'mid', 'leaf')), may hold values from -0.25 to 0.25
- cluster_coupling: bfloat16 [8, 3, 128, 128], P(('top', 'mid')), may hold values from -0.3125 to 0.3125
- group_coupling: bfloat16 [4, 2, 128, 128], P('top'), may hold values from -0.375 to 0.375
- leaf_lists: int32 [256, 4], P(('top', 'mid', 'leaf')), may hold values from 0 to 31, as said below
- owner: int32 [8, 32], P(('top', 'mid')), may hold values from 0 to 31, as said below
- cluster_lists: int32 [8, 3], P(('top', 'mid')), may hold values from 0 to 7, as said below
- group_lists: int32 [4, 2], P('top'), may hold values from 0 to 3, as said below
Outputs:
- solution: bfloat16 [393216, 256], P(('top', 'mid', 'leaf'))
The draws below stay inside these ranges and needn't reach their ends.
Inputs may be any that keep to these rules, and one draw needn't show every extreme that they name: `leaf_lists`: each row holds 4 distinct sibling cluster ids. `owner`: each row is a permutation of the slots of the cluster. `cluster_lists`: each row holds 3 distinct cluster ids. `group_lists`: each row holds 2 distinct group ids. `diag_blocks`: each block is a diagonal with entries from 1 to 3 plus small dense noise.
All inputs are finite; a program needn't handle non-finite values.
Results may differ from the reference program's by a relative error of at most 0.028.
Values may be sent and summed in bfloat16 or wider, within the bound.
A program may use at most 64 MiB of HBM per device.

```python
import jax
import jax.numpy as jnp
from jax import lax

LEAF_N = 1536
RANK = 128
RHS = 256
K0 = 4
K2 = 3
K1 = 2
NTOP = 4
NMID = 8
LEAF_PER = 32
NLEAF = 256
N = 393216


def draw_diag_blocks(key, part):
    first_key, second_key = jax.random.split(jax.random.fold_in(key, 11))
    diagonal = jnp.exp(jax.random.uniform(first_key, (NLEAF, LEAF_N), jnp.float32, 0.0, 1.0986))
    noise_part = jax.random.normal(second_key, (NLEAF, LEAF_N, LEAF_N), jnp.float32) / jnp.sqrt(LEAF_N * 1.0)
    identity = jnp.eye(LEAF_N, dtype=jnp.float32)
    return (noise_part + diagonal[:, :, None] * identity).astype(jnp.bfloat16)


def draw_precond(key, part):
    first_key, second_key = jax.random.split(jax.random.fold_in(key, 23))
    diagonal = jnp.exp(jax.random.uniform(first_key, (NLEAF, LEAF_N), jnp.float32, -1.386, -0.693))
    noise_part = 0.2 * jax.random.normal(second_key, (NLEAF, LEAF_N, LEAF_N), jnp.float32) / jnp.sqrt(LEAF_N * 1.0)
    identity = jnp.eye(LEAF_N, dtype=jnp.float32)
    return (noise_part + diagonal[:, :, None] * identity).astype(jnp.bfloat16)


def distinct_rows(key, salt, rows, choose, total):
    subkeys = jax.random.split(jax.random.fold_in(key, salt), rows)
    return jax.vmap(lambda single: jax.random.permutation(single, total)[:choose])(subkeys).astype(jnp.int32)


def draw_leaf_lists(key, part):
    return distinct_rows(key, 31, NLEAF, K0, LEAF_PER)


def draw_owner(key, part):
    return distinct_rows(key, 37, NMID, LEAF_PER, LEAF_PER)


def draw_cluster_lists(key, part):
    return distinct_rows(key, 41, NMID, K2, NMID)


def draw_group_lists(key, part):
    return distinct_rows(key, 43, NTOP, K1, NTOP)


def block_scale(stream_key, dims, cuts, least, largest):
    level = 1.0
    for axis_at, blocks in cuts:
        draws = jax.random.uniform(jax.random.fold_in(jax.random.fold_in(stream_key, 6), axis_at), (blocks,), jnp.float32, least / len(cuts), largest / len(cuts))
        level = level * jnp.repeat(jnp.exp(draws), dims[axis_at] // blocks).reshape((-1,) + (1,) * (len(dims) - 1 - axis_at))
    return level


def normal_values(stream_key, dims, deviation, limit, cuts=(), kind=jnp.bfloat16):
    array = jax.random.normal(stream_key, dims, jnp.float32) * deviation
    if len(cuts) > 0:
        array = block_scale(stream_key, dims, cuts, -0.22, 0.18) * array
    return jnp.clip(array, min=-limit, max=limit).astype(kind)


def setup_inputs(seed: int = 0) -> dict:
    splits = jax.random.split(jax.random.key(seed), 15)
    rhs = normal_values(splits[0], (N, RHS), 1.0, 6.0, ((0, 256),))
    guess = normal_values(splits[1], (N, RHS), 0.5, 3.0, ((0, 256),))
    diag_blocks = draw_diag_blocks(jax.random.fold_in(splits[14], 71), 0)
    precond = draw_precond(jax.random.fold_in(splits[14], 71), 0)
    bases = normal_values(splits[4], (NLEAF, LEAF_N, RANK), (LEAF_N // 4) ** -0.5, 0.3125, ((0, 256),))
    leaf_to_middle_transfer = normal_values(splits[5], (NLEAF, RANK, RANK), (4 * RANK) ** -0.5, 0.25, ((0, 256),))
    mid_transfer = normal_values(splits[6], (NMID, RANK, RANK), (2 * RANK) ** -0.5, 0.375)
    leaf_coupling = normal_values(splits[7], (NLEAF, K0, RANK, RANK), (RANK * K0) ** -0.5, 0.25, ((0, 256),))
    cluster_coupling = normal_values(splits[8], (NMID, K2, RANK, RANK), (RANK * K2) ** -0.5, 0.3125, ((0, 8),))
    group_coupling = normal_values(splits[9], (NTOP, K1, RANK, RANK), (RANK * K1) ** -0.5, 0.375, ((0, 4),))
    leaf_lists = draw_leaf_lists(jax.random.fold_in(splits[14], 71), 0)
    owner = draw_owner(jax.random.fold_in(splits[14], 71), 0)
    cluster_lists = draw_cluster_lists(jax.random.fold_in(splits[14], 71), 0)
    group_lists = draw_group_lists(jax.random.fold_in(splits[14], 71), 0)
    return {"rhs": rhs, "guess": guess, "diag_blocks": diag_blocks, "precond": precond, "bases": bases, "leaf_to_middle_transfer": leaf_to_middle_transfer, "mid_transfer": mid_transfer, "leaf_coupling": leaf_coupling, "cluster_coupling": cluster_coupling, "group_coupling": group_coupling, "leaf_lists": leaf_lists, "owner": owner, "cluster_lists": cluster_lists, "group_lists": group_lists}


damping = 0.7


def near_part(diag_blocks, blocks):
    def one_block(pair):
        return jnp.dot(pair[0], pair[1], preferred_element_type=jnp.float32)
    return lax.map(one_block, (diag_blocks, blocks))


def apply_matrix(vector, diag_blocks, bases, leaf_to_middle_transfer, mid_transfer, leaf_coupling, cluster_coupling, group_coupling, leaf_lists, owner, cluster_lists, group_lists):
    single_precision = jnp.float32
    brain_float_sixteen = jnp.bfloat16
    blocks = vector.reshape(NLEAF, LEAF_N, RHS)
    leaf_coefficient = jnp.einsum('sna,snr->sar', bases.astype(single_precision), blocks.astype(single_precision)).astype(brain_float_sixteen)
    upward_contribution = jnp.einsum('euw,euk->ewk', leaf_to_middle_transfer.astype(single_precision), leaf_coefficient.astype(single_precision)).astype(brain_float_sixteen)
    cluster_coef = jnp.sum(upward_contribution.astype(single_precision).reshape(NMID, LEAF_PER, RANK, RHS), axis=1).astype(brain_float_sixteen)
    group_terms = jnp.einsum('cba,cbr->car', mid_transfer.astype(single_precision), cluster_coef.astype(single_precision))
    group_coef = jnp.sum(group_terms.reshape(NTOP, NMID // NTOP, RANK, RHS), axis=1).astype(brain_float_sixteen)
    slots = jnp.take_along_axis(owner, leaf_lists.reshape(NMID, LEAF_PER * K0), axis=1)
    leaf_table = leaf_coefficient.reshape(NMID, LEAF_PER, RANK, RHS)
    picked = jax.vmap(lambda table, index: jnp.take(table, index, axis=0))(leaf_table, slots)
    picked = picked.reshape(NLEAF, K0, RANK, RHS)
    leaf_distant_field = jnp.einsum('skab,skbr->sar', leaf_coupling.astype(single_precision), picked.astype(single_precision))
    cluster_far = jnp.einsum('ckab,ckbr->car', cluster_coupling.astype(single_precision), jnp.take(cluster_coef, cluster_lists, axis=0).astype(single_precision))
    group_far = jnp.einsum('gkab,gkbr->gar', group_coupling.astype(single_precision), jnp.take(group_coef, group_lists, axis=0).astype(single_precision)).astype(brain_float_sixteen)
    group_rep = jnp.repeat(group_far, NMID // NTOP, axis=0)
    cluster_total = (cluster_far + jnp.einsum('cab,cbr->car', mid_transfer.astype(single_precision), group_rep.astype(single_precision))).astype(brain_float_sixteen)
    cluster_representative = jnp.repeat(cluster_total, LEAF_PER, axis=0)
    leaf_grand_total = (leaf_distant_field + jnp.einsum('mwo,mon->mwn', leaf_to_middle_transfer.astype(single_precision), cluster_representative.astype(single_precision))).astype(brain_float_sixteen)
    far_part = jnp.einsum('sna,sar->snr', bases.astype(single_precision), leaf_grand_total.astype(single_precision))
    return (near_part(diag_blocks, blocks) + far_part).reshape(N, RHS)


def reference(rhs, guess, diag_blocks, precond, bases, leaf_to_middle_transfer, mid_transfer, leaf_coupling, cluster_coupling, group_coupling, leaf_lists, owner, cluster_lists, group_lists):
    def apply_a(vector):
        return apply_matrix(vector, diag_blocks, bases, leaf_to_middle_transfer, mid_transfer, leaf_coupling, cluster_coupling, group_coupling, leaf_lists, owner, cluster_lists, group_lists)

    def smooth(residual):
        blocks = residual.astype(jnp.bfloat16).reshape(NLEAF, LEAF_N, RHS)
        return near_part(precond, blocks).reshape(N, RHS)

    residual = rhs.astype(jnp.float32) - apply_a(guess)
    first = guess.astype(jnp.float32) + damping * smooth(residual)
    residual = rhs.astype(jnp.float32) - apply_a(first.astype(jnp.bfloat16))
    second = first + damping * smooth(residual)
    return second.astype(jnp.bfloat16)
```

```python
import functools

import jax
import jax.numpy as jnp
from jax import lax
from jax.experimental import pallas as pl
from jax.experimental.pallas import tpu as pltpu
from jax.sharding import PartitionSpec as P

damping = 0.7
MESH = pl.DeviceIdType.MESH
NY, NZ, NC = 4, 8, 8
F32, BF16 = jnp.float32, jnp.bfloat16


def dot_nn(a, b):
    return jnp.dot(a, b, preferred_element_type=F32)


def dot_nt(a, b):
    return lax.dot_general(a, b, (((1,), (1,)), ((), ())), preferred_element_type=F32)


def dot_tn(a, b):
    return lax.dot_general(a, b, (((0,), (0,)), ((), ())), preferred_element_type=F32)


def kernel(
    lists_ref,
    owner_ref,
    clist_ref,
    glist_ref,
    rhs_hbm,
    guess_hbm,
    diag_hbm,
    prec_hbm,
    bases_hbm,
    trans_hbm,
    mid_hbm,
    coup_hbm,
    ccoup_hbm,
    gcoup_hbm,
    out_ref,
    rhs,
    guess,
    diag,
    prec,
    bases,
    trans,
    mid,
    ccoup,
    gcoup,
    coup_all,
    meta_all,
    weights,
    mmat,
    emat,
    rnb,
    first,
    firsth,
    pb,
    gmat,
    w_t,
    acc,
    coef,
    uterm_send,
    uterm_recv,
    row_recv,
    cc_recv,
    ct_all,
    part_send,
    part_recv,
    load_sem,
    wt_send,
    wt_recv,
    ag_send,
    ag_recv,
    rs_send,
    rs_recv,
    ys_send,
    ys_recv,
    cx_send,
    cx_recv,
    ct_send,
    ct_recv,
    pt_send,
    pt_recv,
):
    top, mdl, leaf = lax.axis_index("top"), lax.axis_index("mid"), lax.axis_index("leaf")
    y, z = leaf // NZ, lax.rem(leaf, NZ)
    cluster = top * 2 + mdl
    n, cols = rhs.shape
    rank = bases.shape[1]
    piece = cols // NZ
    tile = n // 6

    def z_peer(dz):
        return (top, mdl, y * NZ + lax.rem(z + dz + NZ, NZ))

    def y_peer(dy):
        return (top, mdl, lax.rem(y + dy, NY) * NZ + z)

    def c_peer(dc):
        other = lax.rem(cluster + dc, NC)
        return (other // 2, lax.rem(other, 2), leaf)

    barrier = pltpu.get_barrier_semaphore()
    for dz in range(1, NZ):
        pl.semaphore_signal(barrier, inc=1, device_id=z_peer(dz), device_id_type=MESH)
    for dy in range(1, NY):
        pl.semaphore_signal(barrier, inc=1, device_id=y_peer(dy), device_id_type=MESH)
    for dc in range(1, NC):
        pl.semaphore_signal(barrier, inc=1, device_id=c_peer(dc), device_id_type=MESH)

    loads = {}
    for i, (name, src, dst) in enumerate(
        (
            ("guess", guess_hbm, guess),
            ("bases", bases_hbm.at[0], bases),
            ("trans", trans_hbm.at[0], trans),
            ("mid", mid_hbm, mid),
            ("ccoup", ccoup_hbm.at[0], ccoup),
            ("gcoup", gcoup_hbm.at[0], gcoup),
            ("coup", coup_hbm.at[0], coup_all.at[0]),
            ("rhs", rhs_hbm, rhs),
            ("diag", diag_hbm.at[0], diag),
            ("prec", prec_hbm.at[0], prec),
        )
    ):
        loads[name] = pltpu.make_async_copy(src, dst, load_sem.at[i])
        loads[name].start()

    sent = []

    def send(src, dst, send_sem, recv_sem, peer):
        copy = pltpu.make_async_remote_copy(
            src_ref=src,
            dst_ref=dst,
            send_sem=send_sem,
            recv_sem=recv_sem,
            device_id=peer,
            device_id_type=MESH,
        )
        copy.start()
        sent.append(copy)

    def arrived(dst, send_sem, recv_sem, peer):
        pltpu.make_async_remote_copy(
            src_ref=dst,
            dst_ref=dst,
            send_sem=send_sem,
            recv_sem=recv_sem,
            device_id=peer,
            device_id_type=MESH,
        ).wait_recv()

    rows = lax.broadcasted_iota(jnp.int32, (8, rank), 0)
    meta = jnp.zeros((8, rank), jnp.int32)
    for k in range(4):
        meta = jnp.where(rows == k, owner_ref[0, lists_ref[0, k]], meta)
    meta_all[0] = meta

    def start_exchange(r, coef_t):
        coef[r, 0] = coef_t
        loads["trans"].wait() if r == 0 else None
        uterm_send[r] = dot_nn(coef_t, trans[...]).astype(BF16)
        if r == 0:
            pl.semaphore_wait(barrier, 2 * (NZ - 1) + NY - 1)
        for dz in (4, 3, 5, 2, 6, 1, 7):
            there = lax.rem(z + dz, NZ)
            send(
                uterm_send.at[r, pl.ds(pl.multiple_of(there * piece, piece), piece)],
                uterm_recv.at[r, NZ - dz],
                rs_send.at[r, dz],
                rs_recv.at[r, NZ - dz],
                z_peer(dz),
            )
        for dz in (2, 6, 1, 7):
            send(
                coef.at[r, 0],
                coef.at[r, NZ - dz],
                ag_send.at[r, dz],
                ag_recv.at[r, NZ - dz],
                z_peer(dz),
            )

    half = cols // 2

    def relay(r):
        arrived(coef.at[r, 6], ag_send.at[r, 2], ag_recv.at[r, 6], z_peer(2))
        send(coef.at[r, 6, pl.ds(0, half)], coef.at[r, 4, pl.ds(0, half)], ag_send.at[r, 4], ag_recv.at[r, 4], z_peer(2))
        send(coef.at[r, 6], coef.at[r, 5], ag_send.at[r, 3], ag_recv.at[r, 5], z_peer(1))
        arrived(coef.at[r, 2], ag_send.at[r, 6], ag_recv.at[r, 2], z_peer(6))
        send(coef.at[r, 2, pl.ds(half, half)], coef.at[r, 4, pl.ds(half, half)], ag_send.at[r, 0], ag_recv.at[r, 0], z_peer(6))
        send(coef.at[r, 2], coef.at[r, 3], ag_send.at[r, 5], ag_recv.at[r, 3], z_peer(7))

    def row_sum(r):
        mine = pl.ds(pl.multiple_of(z * piece, piece), piece)
        total = uterm_send[r, mine].astype(F32)
        for k in range(1, NZ):
            arrived(uterm_recv.at[r, k], rs_send.at[r, NZ - k], rs_recv.at[r, k], z_peer(k))
            total = total + uterm_recv[r, k].astype(F32)
        row_recv[r, 0] = total.astype(BF16)
        for dy in (2, 1, 3):
            send(row_recv.at[r, 0], row_recv.at[r, NY - dy], ys_send.at[r, dy], ys_recv.at[r, NY - dy], y_peer(dy))

    def cluster_sum(r):
        total = row_recv[r, 0].astype(F32)
        for k in range(1, NY):
            arrived(row_recv.at[r, k], ys_send.at[r, NY - k], ys_recv.at[r, k], y_peer(k))
            total = total + row_recv[r, k].astype(F32)
        cc_recv[r, 0] = total.astype(BF16)
        for dc in range(1, NC):
            send(cc_recv.at[r, 0], cc_recv.at[r, NC - dc], cx_send.at[r, dc], cx_recv.at[r, NC - dc], c_peer(dc))

    def cluster_total(r):
        total = dot_nt(cc_recv[r, 0], mmat[0])
        for k in range(1, NC):
            arrived(cc_recv.at[r, k], cx_send.at[r, NC - k], cx_recv.at[r, k], c_peer(k))
            total = total + dot_nt(cc_recv[r, k], mmat[k])
        mine = pl.ds(pl.multiple_of(z * piece, piece), piece)
        ct_all[r, mine] = total.astype(BF16)
        for dz in (4, 3, 5, 2, 6, 1, 7):
            send(ct_all.at[r, mine], ct_all.at[r, mine], ct_send.at[r, dz], ct_recv.at[r, NZ - dz], z_peer(dz))

    def partial_sums(r):
        acc[...] = dot_nt(coef[r, 0], weights[0])
        for k in (2, 6):
            acc[...] += dot_nt(coef[r, k], weights[k])
        for k in (1, 7, 3, 5):
            arrived(coef.at[r, k], ag_send.at[r, NZ - k], ag_recv.at[r, k], z_peer(k))
            acc[...] += dot_nt(coef[r, k], weights[k])
        low, high = coef.at[r, 4, pl.ds(0, half)], coef.at[r, 4, pl.ds(half, half)]
        arrived(low, ag_send.at[r, 4], ag_recv.at[r, 4], z_peer(6))
        arrived(high, ag_send.at[r, 0], ag_recv.at[r, 0], z_peer(2))
        acc[...] += dot_nt(coef[r, 4], weights[4])
        for j in (2, 1, 3):
            part_send[r, j] = acc[:, j * rank : (j + 1) * rank].astype(BF16)
            send(part_send.at[r, j], part_recv.at[r, NY - j], pt_send.at[r, j], pt_recv.at[r, NY - j], y_peer(j))

    def leaf_total(r):
        total = acc[:, 0:rank]
        for k in range(1, NY):
            arrived(part_recv.at[r, k], pt_send.at[r, NY - k], pt_recv.at[r, k], y_peer(k))
            total = total + part_recv[r, k].astype(F32)
        for k in range(1, NZ):
            there = lax.rem(z + k, NZ)
            theirs = ct_all.at[r, pl.ds(pl.multiple_of(there * piece, piece), piece)]
            arrived(theirs, ct_send.at[r, NZ - k], ct_recv.at[r, k], z_peer(k))
        return (total + dot_nt(ct_all[r], trans[...])).astype(BF16)

    loads["guess"].wait()
    loads["bases"].wait()
    start_exchange(0, dot_tn(bases[...], guess[...]).T.astype(BF16))

    for dy in (2, 1, 3):
        send(meta_all.at[0], meta_all.at[NY - dy], wt_send.at[0, dy], wt_recv.at[0, NY - dy], y_peer(dy))
        send(coup_hbm.at[0], coup_all.at[NY - dy], wt_send.at[1, dy], wt_recv.at[1, NY - dy], y_peer(dy))

    loads["mid"].wait()
    loads["gcoup"].wait()
    loads["ccoup"].wait()
    for k in range(2):
        emat[k] = dot_nn(mid[cluster], gcoup[k])

    def compose(k, carry):
        other = lax.rem(cluster + k, NC)
        pick = jnp.zeros((rank, rank), F32)
        for i in range(2):
            pick = pick + jnp.where(glist_ref[0, i] == other // 2, 1.0, 0.0) * emat[i]
        value = dot_nt(pick.astype(BF16), mid[other])
        for i in range(3):
            value = value + jnp.where(clist_ref[0, i] == other, 1.0, 0.0) * ccoup[i].astype(F32)
        mmat[k] = value.astype(BF16)
        return carry

    lax.fori_loop(0, NC, compose, 0)

    loads["rhs"].wait()
    loads["diag"].wait()
    rnb[:, cols : cols + rank] = bases[...]

    def near(i, carry):
        at = pl.ds(pl.multiple_of(i * tile, tile), tile)
        rnb[at, 0:cols] = (rhs[at].astype(F32) - dot_nn(diag[at], guess[...])).astype(BF16)
        return carry

    lax.fori_loop(0, 6, near, 0)
    relay(0)
    row_sum(0)

    loads["prec"].wait()

    def smooth(i, carry):
        at = pl.ds(pl.multiple_of(i * tile, tile), tile)
        both = dot_nn(prec[at], rnb[...])
        base = guess[at].astype(F32) + damping * both[:, 0:cols]
        first[at] = base
        firsth[at] = base.astype(BF16)
        pb[at] = both[:, cols : cols + rank].astype(BF16)
        return carry

    lax.fori_loop(0, 6, smooth, 0)
    cluster_sum(0)

    loads["coup"].wait()
    for k in range(1, NY):
        arrived(meta_all.at[k], wt_send.at[0, NY - k], wt_recv.at[0, k], y_peer(k))
        arrived(coup_all.at[k], wt_send.at[1, NY - k], wt_recv.at[1, k], y_peer(k))

    def place(k, carry):
        slot = y * NZ + lax.rem(z + k, NZ)
        for j in range(NY):
            hit = jnp.where(meta_all[j] == slot, 1.0, 0.0)
            value = jnp.zeros((rank, rank), F32)
            for i in range(4):
                value = value + hit[i : i + 1] * coup_all[j, i].astype(F32)
            weights[k, j * rank : (j + 1) * rank] = value.astype(BF16)
        return carry

    lax.fori_loop(0, NZ, place, 0)
    gmat[...] = dot_tn(bases[...], pb[...]).astype(BF16)
    w_t[...] = dot_tn(bases[...], firsth[...]).T

    partial_sums(0)
    cluster_total(0)
    far = leaf_total(0)

    start_exchange(1, (w_t[...] - damping * dot_nt(far, gmat[...])).astype(BF16))

    def correct(i, carry):
        at = pl.ds(pl.multiple_of(i * tile, tile), tile)
        value = first[at] - damping * dot_nt(pb[at], far)
        first[at] = value
        firsth[at] = value.astype(BF16)
        return carry

    lax.fori_loop(0, 6, correct, 0)

    def near_again(i, carry):
        at = pl.ds(pl.multiple_of(i * tile, tile), tile)
        rnb[at, 0:cols] = (rhs[at].astype(F32) - dot_nn(diag[at], firsth[...])).astype(BF16)
        return carry

    lax.fori_loop(0, 6, near_again, 0)
    relay(1)
    row_sum(1)

    def smooth_again(i, carry):
        at = pl.ds(pl.multiple_of(i * tile, tile), tile)
        first[at] = first[at] + damping * dot_nn(prec[at], rnb[:, 0:cols])
        return carry

    lax.fori_loop(0, 6, smooth_again, 0)
    cluster_sum(1)
    partial_sums(1)
    cluster_total(1)
    far = leaf_total(1)

    def finish(i, carry):
        at = pl.ds(pl.multiple_of(i * tile, tile), tile)
        out_ref[at] = (first[at] - damping * dot_nt(pb[at], far)).astype(BF16)
        return carry

    lax.fori_loop(0, 6, finish, 0)
    for copy in sent:
        copy.wait_send()


def body(
    rhs,
    guess,
    diag_blocks,
    precond,
    bases,
    leaf_to_middle_transfer,
    mid_transfer,
    leaf_coupling,
    cluster_coupling,
    group_coupling,
    leaf_lists,
    owner,
    cluster_lists,
    group_lists,
):
    n, cols = rhs.shape
    rank = bases.shape[2]
    piece = cols // NZ
    smem = pl.BlockSpec(memory_space=pltpu.SMEM)
    hbm = pl.BlockSpec(memory_space=pl.ANY)
    dma = pltpu.SemaphoreType.DMA
    return pl.pallas_call(
        kernel,
        out_shape=jax.ShapeDtypeStruct((n, cols), BF16),
        in_specs=[smem] * 4 + [hbm] * 10,
        out_specs=pl.BlockSpec(memory_space=pltpu.VMEM),
        scratch_shapes=[
            pltpu.VMEM((n, cols), BF16),
            pltpu.VMEM((n, cols), BF16),
            pltpu.VMEM((n, n), BF16),
            pltpu.VMEM((n, n), BF16),
            pltpu.VMEM((n, rank), BF16),
            pltpu.VMEM((rank, rank), BF16),
            pltpu.VMEM((NC, rank, rank), BF16),
            pltpu.VMEM((3, rank, rank), BF16),
            pltpu.VMEM((2, rank, rank), BF16),
            pltpu.VMEM((NY, 4, rank, rank), BF16),
            pltpu.VMEM((NY, 8, rank), jnp.int32),
            pltpu.VMEM((NZ, NY * rank, rank), BF16),
            pltpu.VMEM((NC, rank, rank), BF16),
            pltpu.VMEM((2, rank, rank), F32),
            pltpu.VMEM((n, cols + rank), BF16),
            pltpu.VMEM((n, cols), F32),
            pltpu.VMEM((n, cols), BF16),
            pltpu.VMEM((n, rank), BF16),
            pltpu.VMEM((rank, rank), BF16),
            pltpu.VMEM((cols, rank), F32),
            pltpu.VMEM((cols, NY * rank), F32),
            pltpu.VMEM((2, NZ, cols, rank), BF16),
            pltpu.VMEM((2, cols, rank), BF16),
            pltpu.VMEM((2, NZ, piece, rank), BF16),
            pltpu.VMEM((2, NY, piece, rank), BF16),
            pltpu.VMEM((2, NC, piece, rank), BF16),
            pltpu.VMEM((2, cols, rank), BF16),
            pltpu.VMEM((2, NY, cols, rank), BF16),
            pltpu.VMEM((2, NY, cols, rank), BF16),
            dma((10,)),
            dma((2, NY)),
            dma((2, NY)),
            dma((2, NZ)),
            dma((2, NZ)),
            dma((2, NZ)),
            dma((2, NZ)),
            dma((2, NY)),
            dma((2, NY)),
            dma((2, NC)),
            dma((2, NC)),
            dma((2, NZ)),
            dma((2, NZ)),
            dma((2, NY)),
            dma((2, NY)),
        ],
        compiler_params=pltpu.CompilerParams(
            collective_id=0, has_side_effects=True, vmem_limit_bytes=60 * 1024 * 1024
        ),
    )(
        leaf_lists,
        owner,
        cluster_lists,
        group_lists,
        rhs,
        guess,
        diag_blocks,
        precond,
        bases,
        leaf_to_middle_transfer,
        mid_transfer,
        leaf_coupling,
        cluster_coupling,
        group_coupling,
    )


def solution(mesh):
    in_specs = (
        P(("top", "mid", "leaf"), None),
        P(("top", "mid", "leaf"), None),
        P(("top", "mid", "leaf"), None, None),
        P(("top", "mid", "leaf"), None, None),
        P(("top", "mid", "leaf"), None, None),
        P(("top", "mid", "leaf"), None, None),
        P(),
        P(("top", "mid", "leaf"), None, None, None),
        P(("top", "mid"), None, None, None),
        P("top", None, None, None),
        P(("top", "mid", "leaf"), None),
        P(("top", "mid"), None),
        P(("top", "mid"), None),
        P("top", None),
    )
    out_specs = P(("top", "mid", "leaf"), None)
    return jax.shard_map(body, mesh=mesh, in_specs=in_specs, out_specs=out_specs, check_vma=False)
```

```python
import jax
import jax.numpy as jnp
from jax import lax
from jax.experimental import pallas as pl
from jax.experimental.pallas import tpu as pltpu
from jax.sharding import PartitionSpec as P

damping = 0.7
MESH = pl.DeviceIdType.MESH
NY, NZ, NC = 4, 8, 8
TILES = 3
ABROAD = [(dc, dy) for dc in range(NC) for dy in range(NY) if dc or dy]
COLUMN = [(0, 2), (0, 1), (0, 3)]
PLACE = {0: 0, 1: 1, 7: 2, 2: 3, 6: 4, 3: 5, 5: 6, 4: 7}
F32, BF16 = jnp.float32, jnp.bfloat16


def dot_nn(a, b):
    return jnp.dot(a, b, preferred_element_type=F32)


def dot_nt(a, b):
    return lax.dot_general(a, b, (((1,), (1,)), ((), ())), preferred_element_type=F32)


def dot_tn(a, b):
    return lax.dot_general(a, b, (((0,), (0,)), ((), ())), preferred_element_type=F32)


def kernel(
    lists_hbm,
    owner_hbm,
    clist_hbm,
    glist_hbm,
    rhs_hbm,
    guess_hbm,
    diag_hbm,
    prec_hbm,
    bases_hbm,
    trans_hbm,
    mid_hbm,
    coup_hbm,
    ccoup_hbm,
    gcoup_hbm,
    out_ref,
    lists_ref,
    owner_ref,
    clist_ref,
    glist_ref,
    rhs,
    guess,
    diag,
    prec,
    bases,
    trans,
    mid,
    ccoup,
    gcoup,
    coup_all,
    meta_all,
    weights,
    mmat,
    emat,
    rnb,
    first,
    firsth,
    pb,
    gmat,
    w_t,
    acc,
    coef,
    uterm_send,
    uterm_recv,
    row_recv,
    cc_all,
    ct_all,
    part_send,
    part_recv,
    load_sem,
    wt_send,
    wt_recv,
    ag_send,
    ag_recv,
    rs_send,
    rs_recv,
    ys_send,
    ys_recv,
    cx_send,
    cx_recv,
    ct_send,
    ct_recv,
    pt_send,
    pt_recv,
):
    top, mdl, leaf = lax.axis_index("top"), lax.axis_index("mid"), lax.axis_index("leaf")
    y, z = leaf // NZ, lax.rem(leaf, NZ)
    cluster = top * 2 + mdl
    n, cols = rhs.shape
    rank = bases.shape[1]
    piece = cols // NZ
    half = cols // 2
    tile = n // TILES

    def z_peer(dz):
        return (top, mdl, y * NZ + lax.rem(z + dz, NZ))

    def y_peer(dy):
        return (top, mdl, lax.rem(y + dy, NY) * NZ + z)

    def c_peer(dc, dy):
        other = lax.rem(cluster + dc, NC)
        return (other // 2, lax.rem(other, 2), lax.rem(y + dy, NY) * NZ + z)

    loads = {}
    for i, (name, src, dst) in enumerate(
        (
            ("guess", guess_hbm, guess),
            ("bases", bases_hbm.at[0], bases),
            ("trans", trans_hbm.at[0], trans),
            ("lists", lists_hbm, lists_ref),
            ("owner", owner_hbm, owner_ref),
            ("clist", clist_hbm, clist_ref),
            ("glist", glist_hbm, glist_ref),
            ("rhs", rhs_hbm, rhs),
            ("diag", diag_hbm.at[0], diag),
            ("mid", mid_hbm, mid),
            ("ccoup", ccoup_hbm.at[0], ccoup),
            ("gcoup", gcoup_hbm.at[0], gcoup),
            ("coup", coup_hbm.at[0], coup_all.at[0]),
            ("prec", prec_hbm.at[0], prec),
        )
    ):
        loads[name] = pltpu.make_async_copy(src, dst, load_sem.at[i])
        loads[name].start()

    barrier = pltpu.get_barrier_semaphore()
    for dz in (4, 3, 5, 2, 6, 1, 7):
        pl.semaphore_signal(barrier, inc=1, device_id=z_peer(dz), device_id_type=MESH)
    for dc, dy in ABROAD:
        pl.semaphore_signal(barrier, inc=1, device_id=c_peer(dc, dy), device_id_type=MESH)

    def send(src, dst, send_sem, recv_sem, peer):
        copy = pltpu.make_async_remote_copy(
            src_ref=src,
            dst_ref=dst,
            send_sem=send_sem,
            recv_sem=recv_sem,
            device_id=peer,
            device_id_type=MESH,
        )
        copy.start()

    def arrived(dst, send_sem, recv_sem):
        pltpu.make_async_remote_copy(
            src_ref=dst,
            dst_ref=dst,
            send_sem=send_sem,
            recv_sem=recv_sem,
            device_id=z_peer(1),
            device_id_type=MESH,
        ).wait_recv()

    def left(src, send_sem, recv_sem):
        pltpu.make_async_remote_copy(
            src_ref=src,
            dst_ref=src,
            send_sem=send_sem,
            recv_sem=recv_sem,
            device_id=z_peer(1),
            device_id_type=MESH,
        ).wait_send()

    mine = pl.ds(pl.multiple_of(z * piece, piece), piece)

    def block(r, h, k):
        return coef.at[r, pl.ds(h * half, half), pl.ds(PLACE[k] * rank, rank)]

    def pass_on(r, h, source, k, dz):
        send(block(r, h, source), block(r, h, k), ag_send.at[r], ag_recv.at[r, h, k], z_peer(dz))

    def here(r, h, k):
        arrived(block(r, h, k), ag_send.at[r], ag_recv.at[r, h, k])

    def start_exchange(r, coef_t):
        coef[r, :, 0:rank] = coef_t
        if r == 0:
            loads["trans"].wait()
        uterm_send[r] = dot_nn(coef_t, trans[...]).astype(BF16)
        if r == 0:
            pl.semaphore_wait(barrier, NZ - 1 + len(ABROAD))
        for dz in (4, 3, 5, 2, 6, 1, 7):
            there = lax.rem(z + dz, NZ)
            send(
                uterm_send.at[r, pl.ds(pl.multiple_of(there * piece, piece), piece)],
                uterm_recv.at[r, NZ - dz],
                rs_send.at[r],
                rs_recv.at[r],
                z_peer(dz),
            )
        for dz in (2, 6, 1, 7):
            for h in range(2):
                pass_on(r, h, 0, NZ - dz, dz)

    def relay(r, h):
        here(r, h, 6)
        if h == 0:
            pass_on(r, h, 6, 4, 2)
        pass_on(r, h, 6, 5, 1)
        here(r, h, 2)
        if h == 1:
            pass_on(r, h, 2, 4, 6)
        pass_on(r, h, 2, 3, 7)

    def row_sum(r):
        arrived(uterm_recv.at[r, pl.ds(1, NZ - 1)], rs_send.at[r], rs_recv.at[r])
        total = uterm_send[r, mine].astype(F32)
        for k in range(1, NZ):
            total = total + uterm_recv[r, k].astype(F32)
        row_recv[r, 0] = total.astype(BF16)
        for dc, dy in ABROAD if r else COLUMN:
            k = (NC - dc) % NC * NY + (NY - dy) % NY
            send(row_recv.at[r, 0], row_recv.at[r, k], ys_send.at[r], ys_recv.at[r], c_peer(dc, dy))

    def cluster_sum(r, k):
        total = row_recv[r, k * NY].astype(F32)
        for dy in range(1, NY):
            total = total + row_recv[r, k * NY + dy].astype(F32)
        cc_all[r, :, k * rank : (k + 1) * rank] = total.astype(BF16)

    def pass_sum():
        arrived(row_recv.at[0, pl.ds(1, NY - 1)], ys_send.at[0], ys_recv.at[0])
        cluster_sum(0, 0)
        for dc in range(1, NC):
            there = cc_all.at[0, :, pl.ds((NC - dc) * rank, rank)]
            send(cc_all.at[0, :, pl.ds(0, rank)], there, cx_send, cx_recv, c_peer(dc, 0))

    def cluster_total(r):
        if r == 0:
            arrived(cc_all.at[0, :, pl.ds(rank, (NC - 1) * rank)], cx_send, cx_recv)
        else:
            arrived(row_recv.at[r, pl.ds(1, NC * NY - 1)], ys_send.at[r], ys_recv.at[r])
            for k in range(NC):
                cluster_sum(r, k)
        ct_all[r, mine] = dot_nt(cc_all[r], mmat[...]).astype(BF16)
        for dz in (4, 3, 5, 2, 6, 1, 7):
            send(ct_all.at[r, mine], ct_all.at[r, mine], ct_send.at[r], ct_recv.at[r], z_peer(dz))

    def early_sums(r):
        for h in range(2):
            here(r, h, 1)
            here(r, h, 7)
        acc[...] = dot_nt(coef[r, :, 0 : 5 * rank], weights[:, 0 : 5 * rank])

    def late_sums(r, h):
        for k in (3, 5, 4):
            here(r, h, k)
        rows = slice(h * half, (h + 1) * half)
        value = acc[rows] + dot_nt(coef[r, rows, 5 * rank :], weights[:, 5 * rank :])
        acc[rows, 0:rank] = value[:, 0:rank]
        for j in (2, 1, 3):
            part_send[r, j, rows] = value[:, j * rank : (j + 1) * rank].astype(BF16)
        for j in (2, 1, 3):
            send(
                part_send.at[r, j, pl.ds(h * half, half)],
                part_recv.at[r, h, NY - j],
                pt_send.at[r],
                pt_recv.at[r, h],
                y_peer(j),
            )

    def leaf_total(r):
        for h in range(2):
            arrived(part_recv.at[r, h, pl.ds(1, NY - 1)], pt_send.at[r], pt_recv.at[r, h])
        totals = []
        for h in range(2):
            total = acc[h * half : (h + 1) * half, 0:rank]
            for k in range(1, NY):
                total = total + part_recv[r, h, k].astype(F32)
            totals.append(total)
        total = jnp.concatenate(totals, axis=0)
        arrived(ct_all.at[r, pl.ds(0, cols - piece)], ct_send.at[r], ct_recv.at[r])
        return (total + dot_nt(ct_all[r], trans[...])).astype(BF16)

    def all_left(r):
        left(uterm_send.at[r, pl.ds(0, cols - piece)], rs_send.at[r], rs_recv.at[r])
        left(coef.at[r, :, pl.ds(0, 7 * rank)], ag_send.at[r], ag_recv.at[r, 0, 0])
        if r == 0:
            left(row_recv.at[r, pl.ds(1, NY - 1)], ys_send.at[r], ys_recv.at[r])
            left(cc_all.at[r, :, pl.ds(rank, (NC - 1) * rank)], cx_send, cx_recv)
        else:
            left(row_recv.at[r, pl.ds(1, NC * NY - 1)], ys_send.at[r], ys_recv.at[r])
        left(ct_all.at[r, pl.ds(0, cols - piece)], ct_send.at[r], ct_recv.at[r])
        left(part_send.at[r, pl.ds(1, NY - 1)], pt_send.at[r], pt_recv.at[r, 0])

    def tiles(step, begin=0, end=TILES):
        def run(i, carry):
            step(pl.ds(pl.multiple_of(i * tile, tile), tile))
            return carry

        lax.fori_loop(begin, end, run, 0)

    loads["guess"].wait()
    loads["bases"].wait()
    start_exchange(0, dot_tn(bases[...], guess[...]).T.astype(BF16))

    loads["lists"].wait()
    loads["owner"].wait()
    rows = lax.broadcasted_iota(jnp.int32, (8, rank), 0)
    meta = jnp.zeros((8, rank), jnp.int32)
    for k in range(4):
        meta = jnp.where(rows == k, owner_ref[0, lists_ref[0, k]], meta)
    meta_all[0] = meta
    for dy in (2, 1, 3):
        send(coup_hbm.at[0], coup_all.at[NY - dy], wt_send.at[1], wt_recv.at[1], y_peer(dy))
        send(meta_all.at[0], meta_all.at[NY - dy], wt_send.at[0], wt_recv.at[0], y_peer(dy))

    loads["rhs"].wait()
    loads["diag"].wait()
    rnb[:, cols : cols + rank] = bases[...]

    def near(at):
        rnb[at, 0:cols] = (rhs[at].astype(F32) - dot_nn(diag[at], guess[...])).astype(BF16)

    tiles(near)

    for name in ("mid", "gcoup", "ccoup", "clist", "glist"):
        loads[name].wait()
    for k in range(2):
        emat[k] = dot_nn(mid[cluster], gcoup[k])

    def compose(k, carry):
        other = lax.rem(cluster + k, NC)
        pick = jnp.zeros((rank, rank), F32)
        for i in range(2):
            pick = pick + jnp.where(glist_ref[0, i] == other // 2, 1.0, 0.0) * emat[i]
        value = dot_nt(pick.astype(BF16), mid[other])
        for i in range(3):
            value = value + jnp.where(clist_ref[0, i] == other, 1.0, 0.0) * ccoup[i].astype(F32)
        mmat[:, pl.ds(pl.multiple_of(k * rank, rank), rank)] = value.astype(BF16)
        return carry

    lax.fori_loop(0, NC, compose, 0)

    row_sum(0)
    relay(0, 0)
    relay(0, 1)

    loads["prec"].wait()

    def smooth(at):
        both = dot_nn(prec[at], rnb[...])
        base = guess[at].astype(F32) + damping * both[:, 0:cols]
        first[at] = base
        firsth[at] = base.astype(BF16)
        pb[at] = both[:, cols : cols + rank].astype(BF16)

    tiles(smooth, 0, 1)
    pass_sum()

    loads["coup"].wait()
    arrived(meta_all.at[pl.ds(1, NY - 1)], wt_send.at[0], wt_recv.at[0])
    arrived(coup_all.at[pl.ds(1, NY - 1)], wt_send.at[1], wt_recv.at[1])

    def place(p, carry):
        away = ((p + 1) // 2) * (2 * lax.rem(p, 2) - 1)
        slot = y * NZ + lax.rem(z + away + NZ, NZ)
        for j in range(NY):
            hit = jnp.where(meta_all[j] == slot, 1.0, 0.0)
            value = jnp.zeros((rank, rank), F32)
            for i in range(4):
                value = value + hit[i : i + 1] * coup_all[j, i].astype(F32)
            weights[j * rank : (j + 1) * rank, pl.ds(pl.multiple_of(p * rank, rank), rank)] = value.astype(BF16)
        return carry

    lax.fori_loop(0, NZ, place, 0)
    early_sums(0)
    tiles(smooth, 1, 2)
    late_sums(0, 0)
    late_sums(0, 1)
    cluster_total(0)
    tiles(smooth, 2, 3)
    gmat[...] = dot_tn(bases[...], pb[...]).astype(BF16)
    w_t[...] = dot_tn(bases[...], firsth[...]).T
    far = leaf_total(0)

    start_exchange(1, (w_t[...] - damping * dot_nt(far, gmat[...])).astype(BF16))

    def correct(at):
        value = first[at] - damping * dot_nt(pb[at], far)
        first[at] = value
        firsth[at] = value.astype(BF16)

    correct(slice(0, n))

    def near_again(at):
        rnb[at, 0:cols] = (rhs[at].astype(F32) - dot_nn(diag[at], firsth[...])).astype(BF16)

    tiles(near_again)
    row_sum(1)
    relay(1, 0)
    relay(1, 1)

    def smooth_again(at):
        first[at] = first[at] + damping * dot_nn(prec[at], rnb[:, 0:cols])

    tiles(smooth_again)
    early_sums(1)
    late_sums(1, 0)
    late_sums(1, 1)
    cluster_total(1)
    all_left(0)
    left(meta_all.at[pl.ds(1, NY - 1)], wt_send.at[0], wt_recv.at[0])
    left(coup_all.at[pl.ds(1, NY - 1)], wt_send.at[1], wt_recv.at[1])
    far = leaf_total(1)

    def finish(at):
        out_ref[at] = (first[at] - damping * dot_nt(pb[at], far)).astype(BF16)

    finish(slice(0, n))
    all_left(1)


def body(
    rhs,
    guess,
    diag_blocks,
    precond,
    bases,
    leaf_to_middle_transfer,
    mid_transfer,
    leaf_coupling,
    cluster_coupling,
    group_coupling,
    leaf_lists,
    owner,
    cluster_lists,
    group_lists,
):
    n, cols = rhs.shape
    rank = bases.shape[2]
    piece = cols // NZ
    hbm = pl.BlockSpec(memory_space=pltpu.HBM)
    dma = pltpu.SemaphoreType.DMA
    return pl.pallas_call(
        kernel,
        out_shape=pltpu.VMEM((n, cols), BF16),
        in_specs=[hbm] * 14,
        out_specs=pl.BlockSpec(memory_space=pltpu.VMEM),
        scratch_shapes=[
            pltpu.SMEM(leaf_lists.shape, jnp.int32),
            pltpu.SMEM(owner.shape, jnp.int32),
            pltpu.SMEM(cluster_lists.shape, jnp.int32),
            pltpu.SMEM(group_lists.shape, jnp.int32),
            pltpu.VMEM((n, cols), BF16),
            pltpu.VMEM((n, cols), BF16),
            pltpu.VMEM((n, n), BF16),
            pltpu.VMEM((n, n), BF16),
            pltpu.VMEM((n, rank), BF16),
            pltpu.VMEM((rank, rank), BF16),
            pltpu.VMEM((NC, rank, rank), BF16),
            pltpu.VMEM((3, rank, rank), BF16),
            pltpu.VMEM((2, rank, rank), BF16),
            pltpu.VMEM((NY, 4, rank, rank), BF16),
            pltpu.VMEM((NY, 8, rank), jnp.int32),
            pltpu.VMEM((NY * rank, NZ * rank), BF16),
            pltpu.VMEM((rank, NC * rank), BF16),
            pltpu.VMEM((2, rank, rank), F32),
            pltpu.VMEM((n, cols + rank), BF16),
            pltpu.VMEM((n, cols), F32),
            pltpu.VMEM((n, cols), BF16),
            pltpu.VMEM((n, rank), BF16),
            pltpu.VMEM((rank, rank), BF16),
            pltpu.VMEM((cols, rank), F32),
            pltpu.VMEM((cols, NY * rank), F32),
            pltpu.VMEM((2, cols, NZ * rank), BF16),
            pltpu.VMEM((2, cols, rank), BF16),
            pltpu.VMEM((2, NZ, piece, rank), BF16),
            pltpu.VMEM((2, NC * NY, piece, rank), BF16),
            pltpu.VMEM((2, piece, NC * rank), BF16),
            pltpu.VMEM((2, cols, rank), BF16),
            pltpu.VMEM((2, NY, cols, rank), BF16),
            pltpu.VMEM((2, 2, NY, cols // 2, rank), BF16),
            dma((14,)),
            dma((2,)),
            dma((2,)),
            dma((2,)),
            dma((2, 2, NZ)),
            dma((2,)),
            dma((2,)),
            dma((2,)),
            dma((2,)),
            dma,
            dma,
            dma((2,)),
            dma((2,)),
            dma((2,)),
            dma((2, 2)),
        ],
        compiler_params=pltpu.CompilerParams(
            collective_id=0, has_side_effects=True, vmem_limit_bytes=67043328 - n * cols * 2
        ),
    )(
        leaf_lists,
        owner,
        cluster_lists,
        group_lists,
        rhs,
        guess,
        diag_blocks,
        precond,
        bases,
        leaf_to_middle_transfer,
        mid_transfer,
        leaf_coupling,
        cluster_coupling,
        group_coupling,
    )


def solution(mesh):
    in_specs = (
        P(("top", "mid", "leaf"), None),
        P(("top", "mid", "leaf"), None),
        P(("top", "mid", "leaf"), None, None),
        P(("top", "mid", "leaf"), None, None),
        P(("top", "mid", "leaf"), None, None),
        P(("top", "mid", "leaf"), None, None),
        P(),
        P(("top", "mid", "leaf"), None, None, None),
        P(("top", "mid"), None, None, None),
        P("top", None, None, None),
        P(("top", "mid", "leaf"), None),
        P(("top", "mid"), None),
        P(("top", "mid"), None),
        P("top", None),
    )
    out_specs = P(("top", "mid", "leaf"), None)
    return jax.shard_map(body, mesh=mesh, in_specs=in_specs, out_specs=out_specs, check_vma=False)
```

```python
import jax
import jax.numpy as jnp
from jax import lax
from jax.experimental import pallas as pl
from jax.experimental.pallas import tpu as pltpu
from jax.sharding import PartitionSpec as P

damping = 0.7
MESH = pl.DeviceIdType.MESH
NY, NZ, NC = 4, 8, 8
TILES = 3
ABROAD = [(k, dy) for k in range(NC) for dy in range(NY) if k or dy]
ABROAD.sort(key=lambda p: -((0, 2, 0, 2, 1, 1, 1, 1)[p[0]] + (0, 1, 2, 1)[p[1]]))
PLACE = {0: 0, 1: 1, 7: 2, 2: 3, 6: 4, 3: 5, 5: 6, 4: 7}
F32, BF16 = jnp.float32, jnp.bfloat16


def dot_nn(a, b):
    return jnp.dot(a, b, preferred_element_type=F32)


def dot_nt(a, b):
    return lax.dot_general(a, b, (((1,), (1,)), ((), ())), preferred_element_type=F32)


def dot_tn(a, b):
    return lax.dot_general(a, b, (((0,), (0,)), ((), ())), preferred_element_type=F32)


def kernel(
    lists_hbm,
    owner_hbm,
    clist_hbm,
    glist_hbm,
    rhs_hbm,
    guess_hbm,
    diag_hbm,
    prec_hbm,
    bases_hbm,
    trans_hbm,
    mid_hbm,
    coup_hbm,
    ccoup_hbm,
    gcoup_hbm,
    out_ref,
    lists_ref,
    owner_ref,
    clist_ref,
    glist_ref,
    rhs,
    guess,
    diag,
    prec,
    trans,
    mid,
    ccoup,
    gcoup,
    coup_all,
    meta_all,
    weights,
    mmat,
    emat,
    rnb,
    first,
    firsth,
    pbx,
    gmat,
    w_t,
    acc,
    coef,
    uterm_send,
    uterm_recv,
    row_recv,
    cc_all,
    far,
    part_send,
    part_recv,
    load_sem,
    wt_send,
    wt_recv,
    ag_send,
    ag_recv,
    rs_send,
    rs_recv,
    ys_send,
    ys_recv,
    cx_send,
    cx_recv,
    ct_send,
    ct_recv,
    pt_send,
    pt_recv,
):
    top, mdl, leaf = lax.axis_index("top"), lax.axis_index("mid"), lax.axis_index("leaf")
    y, z = leaf // NZ, lax.rem(leaf, NZ)
    cluster = top * 2 + mdl
    n, cols = rhs.shape
    rank = trans.shape[1]
    piece = cols // NZ
    half = cols // 2
    tile = n // TILES

    def z_peer(dz):
        return (top, mdl, y * NZ + lax.rem(z + dz, NZ))

    def y_peer(dy):
        return (top, mdl, lax.rem(y + dy, NY) * NZ + z)

    def flipped(k):
        high = lax.rem(top // 2 + k // 4, 2)
        low = lax.rem(lax.rem(top, 2) + k // 2 % 2, 2)
        return high * 2 + low, lax.rem(mdl + k % 2, 2)

    def c_peer(k, dy):
        return (*flipped(k), lax.rem(y + dy, NY) * NZ + z)

    barrier = pltpu.get_barrier_semaphore()
    for dz in (4, 3, 5, 2, 6, 1, 7):
        pl.semaphore_signal(barrier, inc=1, device_id=z_peer(dz), device_id_type=MESH)
    for dc, dy in ABROAD:
        pl.semaphore_signal(barrier, inc=1, device_id=c_peer(dc, dy), device_id_type=MESH)

    loads = {}
    for i, (name, src, dst) in enumerate(
        (
            ("bases", bases_hbm.at[0], rnb.at[:, pl.ds(0, rank)]),
            ("trans", trans_hbm.at[0], trans),
            ("guess", guess_hbm, guess),
            ("lists", lists_hbm, lists_ref),
            ("owner", owner_hbm, owner_ref),
            ("clist", clist_hbm, clist_ref),
            ("glist", glist_hbm, glist_ref),
            ("rhs", rhs_hbm, rhs),
            ("diag", diag_hbm.at[0], diag),
            ("mid", mid_hbm, mid),
            ("ccoup", ccoup_hbm.at[0], ccoup),
            ("gcoup", gcoup_hbm.at[0], gcoup),
            ("coup", coup_hbm.at[0], coup_all.at[0]),
            ("prec", prec_hbm.at[0], prec),
        )
    ):
        loads[name] = pltpu.make_async_copy(src, dst, load_sem.at[i])
        loads[name].start()

    def send(src, dst, send_sem, recv_sem, peer):
        copy = pltpu.make_async_remote_copy(
            src_ref=src,
            dst_ref=dst,
            send_sem=send_sem,
            recv_sem=recv_sem,
            device_id=peer,
            device_id_type=MESH,
        )
        copy.start()

    def arrived(dst, send_sem, recv_sem):
        pltpu.make_async_remote_copy(
            src_ref=dst,
            dst_ref=dst,
            send_sem=send_sem,
            recv_sem=recv_sem,
            device_id=z_peer(1),
            device_id_type=MESH,
        ).wait_recv()

    def left(src, send_sem, recv_sem):
        pltpu.make_async_remote_copy(
            src_ref=src,
            dst_ref=src,
            send_sem=send_sem,
            recv_sem=recv_sem,
            device_id=z_peer(1),
            device_id_type=MESH,
        ).wait_send()

    mine = pl.ds(pl.multiple_of(z * piece, piece), piece)

    def block(r, h, k):
        return coef.at[r, pl.ds(h * half, half), pl.ds(PLACE[k] * rank, rank)]

    def pass_on(r, h, source, k, dz):
        send(block(r, h, source), block(r, h, k), ag_send.at[r], ag_recv.at[r, h, k], z_peer(dz))

    def here(r, h, k):
        arrived(block(r, h, k), ag_send.at[r], ag_recv.at[r, h, k])

    def start_exchange(r, both):
        coef[r, :, 0:rank] = both[:, 0:rank].astype(BF16)
        uterm_send[r] = both[:, rank:].astype(BF16)
        if r == 0:
            pl.semaphore_wait(barrier, NZ - 1 + len(ABROAD))
        for dz in (4, 3, 5, 2, 6, 1, 7):
            there = lax.rem(z + dz, NZ)
            send(
                uterm_send.at[r, pl.ds(pl.multiple_of(there * piece, piece), piece)],
                uterm_recv.at[r, NZ - dz],
                rs_send.at[r],
                rs_recv.at[r],
                z_peer(dz),
            )
        for dz in (2, 6, 1, 7):
            for h in range(2):
                pass_on(r, h, 0, NZ - dz, dz)

    def relay(r, h):
        here(r, h, 6)
        if h == 0:
            pass_on(r, h, 6, 4, 2)
        pass_on(r, h, 6, 5, 1)
        here(r, h, 2)
        if h == 1:
            pass_on(r, h, 2, 4, 6)
        pass_on(r, h, 2, 3, 7)

    def row_sum(r):
        arrived(uterm_recv.at[r, pl.ds(1, NZ - 1)], rs_send.at[r], rs_recv.at[r])
        total = uterm_send[r, mine].astype(F32)
        for k in range(1, NZ):
            total = total + uterm_recv[r, k].astype(F32)
        if r == 0:
            cc_all[0, :, 0:rank] = total.astype(BF16)
            for k in (1, 3, 4, 5, 6, 7, 2):
                there = cc_all.at[0, :, pl.ds(k * rank, rank)]
                send(cc_all.at[0, :, pl.ds(0, rank)], there, cx_send, cx_recv, c_peer(k, 0))
        else:
            row_recv[1, 0] = total.astype(BF16)
            for k, dy in ABROAD:
                there = row_recv.at[1, k * NY + (NY - dy) % NY]
                send(row_recv.at[1, 0], there, ys_send.at[1], ys_recv.at[1], c_peer(k, dy))

    def column_sum(r, k):
        total = row_recv[r, k * NY].astype(F32)
        for dy in range(1, NY):
            total = total + row_recv[r, k * NY + dy].astype(F32)
        return total

    def pass_sum():
        arrived(cc_all.at[0, :, pl.ds(rank, (NC - 1) * rank)], cx_send, cx_recv)
        row_recv[0, 0] = dot_nt(cc_all[0], mmat[...]).astype(BF16)
        for dy in (2, 1, 3):
            send(row_recv.at[0, 0], row_recv.at[0, NY - dy], ys_send.at[0], ys_recv.at[0], y_peer(dy))

    def cluster_total(r):
        if r == 0:
            arrived(row_recv.at[0, pl.ds(1, NY - 1)], ys_send.at[0], ys_recv.at[0])
            total = column_sum(0, 0)
        else:
            arrived(row_recv.at[1, pl.ds(1, NC * NY - 1)], ys_send.at[1], ys_recv.at[1])
            for k in range(NC):
                cc_all[1, :, k * rank : (k + 1) * rank] = column_sum(1, k).astype(BF16)
            total = dot_nt(cc_all[1], mmat[...])
        far[r, mine, rank:] = total.astype(BF16)
        there = far.at[r, mine, pl.ds(rank, rank)]
        for dz in (4, 3, 5, 2, 6, 1, 7):
            send(there, there, ct_send.at[r], ct_recv.at[r], z_peer(dz))

    def early_sums(r):
        for h in range(2):
            here(r, h, 1)
            here(r, h, 7)
        acc[...] = dot_nt(coef[r, :, 0 : 5 * rank], weights[:, 0 : 5 * rank])

    def late_sums(r, h):
        for k in (3, 5, 4):
            here(r, h, k)
        rows = slice(h * half, (h + 1) * half)
        value = acc[rows] + dot_nt(coef[r, rows, 5 * rank :], weights[:, 5 * rank :])
        acc[rows, 0:rank] = value[:, 0:rank]
        for j in (2, 1, 3):
            part_send[r, j, rows] = value[:, j * rank : (j + 1) * rank].astype(BF16)
        for j in (2, 1, 3):
            send(
                part_send.at[r, j, pl.ds(h * half, half)],
                part_recv.at[r, h, NY - j],
                pt_send.at[r],
                pt_recv.at[r, h],
                y_peer(j),
            )

    def leaf_total(r):
        for h in range(2):
            arrived(part_recv.at[r, h, pl.ds(1, NY - 1)], pt_send.at[r], pt_recv.at[r, h])
        for h in range(2):
            at = slice(h * half, (h + 1) * half)
            total = acc[at, 0:rank]
            for k in range(1, NY):
                total = total + part_recv[r, h, k].astype(F32)
            far[r, at, 0:rank] = total.astype(BF16)
        arrived(far.at[r, pl.ds(0, cols - piece), pl.ds(rank, rank)], ct_send.at[r], ct_recv.at[r])

    def all_left(r):
        left(uterm_send.at[r, pl.ds(0, cols - piece)], rs_send.at[r], rs_recv.at[r])
        left(coef.at[r, :, pl.ds(0, 7 * rank)], ag_send.at[r], ag_recv.at[r, 0, 0])
        if r == 0:
            left(row_recv.at[r, pl.ds(1, NY - 1)], ys_send.at[r], ys_recv.at[r])
            left(cc_all.at[r, :, pl.ds(rank, (NC - 1) * rank)], cx_send, cx_recv)
        else:
            left(row_recv.at[r, pl.ds(1, NC * NY - 1)], ys_send.at[r], ys_recv.at[r])
        left(far.at[r, pl.ds(0, cols - piece), pl.ds(rank, rank)], ct_send.at[r], ct_recv.at[r])
        left(part_send.at[r, pl.ds(1, NY - 1)], pt_send.at[r], pt_recv.at[r, 0])

    def tiles(step, begin=0, end=TILES):
        def run(i, carry):
            step(pl.ds(pl.multiple_of(i * tile, tile), tile))
            return carry

        lax.fori_loop(begin, end, run, 0)

    loads["bases"].wait()
    loads["trans"].wait()
    rnb[:, rank : 2 * rank] = dot_nn(rnb[:, 0:rank], trans[...]).astype(BF16)
    bases = rnb.at[:, pl.ds(0, 2 * rank)]
    loads["guess"].wait()
    start_exchange(0, dot_tn(guess[...], bases[...]))

    loads["lists"].wait()
    loads["owner"].wait()
    rows = lax.broadcasted_iota(jnp.int32, (8, rank), 0)
    meta = jnp.zeros((8, rank), jnp.int32)
    for k in range(4):
        meta = jnp.where(rows == k, owner_ref[0, lists_ref[0, k]], meta)
    meta_all[0] = meta
    for dy in (2, 1, 3):
        send(coup_hbm.at[0], coup_all.at[NY - dy], wt_send.at[1], wt_recv.at[1], y_peer(dy))
        send(meta_all.at[0], meta_all.at[NY - dy], wt_send.at[0], wt_recv.at[0], y_peer(dy))

    loads["rhs"].wait()
    loads["diag"].wait()

    def near(at):
        rnb[at, 2 * rank :] = (rhs[at].astype(F32) - dot_nn(diag[at], guess[...])).astype(BF16)

    tiles(near)

    for name in ("mid", "gcoup", "ccoup", "clist", "glist"):
        loads[name].wait()
    for k in range(2):
        emat[k] = dot_nn(mid[cluster], gcoup[k])

    def compose(k, carry):
        there, also = flipped(k)
        other = there * 2 + also
        pick = jnp.zeros((rank, rank), F32)
        for i in range(2):
            pick = pick + jnp.where(glist_ref[0, i] == there, 1.0, 0.0) * emat[i]
        value = dot_nt(pick.astype(BF16), mid[other])
        for i in range(3):
            value = value + jnp.where(clist_ref[0, i] == other, 1.0, 0.0) * ccoup[i].astype(F32)
        mmat[:, pl.ds(pl.multiple_of(k * rank, rank), rank)] = value.astype(BF16)
        return carry

    lax.fori_loop(0, NC, compose, 0)

    row_sum(0)
    relay(0, 0)
    relay(0, 1)
    pass_sum()

    loads["coup"].wait()
    arrived(meta_all.at[pl.ds(1, NY - 1)], wt_send.at[0], wt_recv.at[0])
    arrived(coup_all.at[pl.ds(1, NY - 1)], wt_send.at[1], wt_recv.at[1])

    def place(p, carry):
        away = ((p + 1) // 2) * (2 * lax.rem(p, 2) - 1)
        slot = y * NZ + lax.rem(z + away + NZ, NZ)
        for j in range(NY):
            hit = jnp.where(meta_all[j] == slot, 1.0, 0.0)
            value = jnp.zeros((rank, rank), F32)
            for i in range(4):
                value = value + hit[i : i + 1] * coup_all[j, i].astype(F32)
            weights[j * rank : (j + 1) * rank, pl.ds(pl.multiple_of(p * rank, rank), rank)] = value.astype(BF16)
        return carry

    lax.fori_loop(0, NZ, place, 0)
    early_sums(0)
    late_sums(0, 0)
    late_sums(0, 1)
    cluster_total(0)

    loads["prec"].wait()

    def smooth(at):
        both = dot_nn(prec[at], rnb[...])
        base = guess[at].astype(F32) + damping * both[:, 2 * rank :]
        first[at] = base
        firsth[at] = base.astype(BF16)
        pbx[at] = both[:, 0 : 2 * rank].astype(BF16)

    tiles(smooth)
    gmat[...] = dot_tn(bases[...], pbx[...]).astype(BF16)
    w_t[...] = dot_tn(firsth[...], bases[...])
    leaf_total(0)

    start_exchange(1, w_t[...] - damping * dot_nt(far[0], gmat[...]))

    def correct(at):
        value = first[at] - damping * dot_nt(pbx[at], far[0])
        first[at] = value
        firsth[at] = value.astype(BF16)

    correct(slice(0, n))

    def near_again(at):
        rnb[at, 2 * rank :] = (rhs[at].astype(F32) - dot_nn(diag[at], firsth[...])).astype(BF16)

    tiles(near_again)
    row_sum(1)
    relay(1, 0)
    relay(1, 1)

    def smooth_again(at):
        first[at] = first[at] + damping * dot_nn(prec[at], rnb[:, 2 * rank :])

    tiles(smooth_again)
    early_sums(1)
    late_sums(1, 0)
    late_sums(1, 1)
    cluster_total(1)
    all_left(0)
    left(meta_all.at[pl.ds(1, NY - 1)], wt_send.at[0], wt_recv.at[0])
    left(coup_all.at[pl.ds(1, NY - 1)], wt_send.at[1], wt_recv.at[1])
    leaf_total(1)

    def finish(at):
        out_ref[at] = (first[at] - damping * dot_nt(pbx[at], far[1])).astype(BF16)

    finish(slice(0, n))
    all_left(1)


def body(
    rhs,
    guess,
    diag_blocks,
    precond,
    bases,
    leaf_to_middle_transfer,
    mid_transfer,
    leaf_coupling,
    cluster_coupling,
    group_coupling,
    leaf_lists,
    owner,
    cluster_lists,
    group_lists,
):
    n, cols = rhs.shape
    rank = bases.shape[2]
    piece = cols // NZ
    hbm = pl.BlockSpec(memory_space=pltpu.HBM)
    dma = pltpu.SemaphoreType.DMA
    return pl.pallas_call(
        kernel,
        out_shape=pltpu.VMEM((n, cols), BF16),
        in_specs=[hbm] * 14,
        out_specs=pl.BlockSpec(memory_space=pltpu.VMEM),
        scratch_shapes=[
            pltpu.SMEM(leaf_lists.shape, jnp.int32),
            pltpu.SMEM(owner.shape, jnp.int32),
            pltpu.SMEM(cluster_lists.shape, jnp.int32),
            pltpu.SMEM(group_lists.shape, jnp.int32),
            pltpu.VMEM((n, cols), BF16),
            pltpu.VMEM((n, cols), BF16),
            pltpu.VMEM((n, n), BF16),
            pltpu.VMEM((n, n), BF16),
            pltpu.VMEM((rank, rank), BF16),
            pltpu.VMEM((NC, rank, rank), BF16),
            pltpu.VMEM((3, rank, rank), BF16),
            pltpu.VMEM((2, rank, rank), BF16),
            pltpu.VMEM((NY, 4, rank, rank), BF16),
            pltpu.VMEM((NY, 8, rank), jnp.int32),
            pltpu.VMEM((NY * rank, NZ * rank), BF16),
            pltpu.VMEM((rank, NC * rank), BF16),
            pltpu.VMEM((2, rank, rank), F32),
            pltpu.VMEM((n, cols + 2 * rank), BF16),
            pltpu.VMEM((n, cols), F32),
            pltpu.VMEM((n, cols), BF16),
            pltpu.VMEM((n, 2 * rank), BF16),
            pltpu.VMEM((2 * rank, 2 * rank), BF16),
            pltpu.VMEM((cols, 2 * rank), F32),
            pltpu.VMEM((cols, NY * rank), F32),
            pltpu.VMEM((2, cols, NZ * rank), BF16),
            pltpu.VMEM((2, cols, rank), BF16),
            pltpu.VMEM((2, NZ, piece, rank), BF16),
            pltpu.VMEM((2, NC * NY, piece, rank), BF16),
            pltpu.VMEM((2, piece, NC * rank), BF16),
            pltpu.VMEM((2, cols, 2 * rank), BF16),
            pltpu.VMEM((2, NY, cols, rank), BF16),
            pltpu.VMEM((2, 2, NY, cols // 2, rank), BF16),
            dma((14,)),
            dma((2,)),
            dma((2,)),
            dma((2,)),
            dma((2, 2, NZ)),
            dma((2,)),
            dma((2,)),
            dma((2,)),
            dma((2,)),
            dma,
            dma,
            dma((2,)),
            dma((2,)),
            dma((2,)),
            dma((2, 2)),
        ],
        compiler_params=pltpu.CompilerParams(
            collective_id=0, has_side_effects=True, vmem_limit_bytes=67043328 - n * cols * 2
        ),
    )(
        leaf_lists,
        owner,
        cluster_lists,
        group_lists,
        rhs,
        guess,
        diag_blocks,
        precond,
        bases,
        leaf_to_middle_transfer,
        mid_transfer,
        leaf_coupling,
        cluster_coupling,
        group_coupling,
    )


def solution(mesh):
    in_specs = (
        P(("top", "mid", "leaf"), None),
        P(("top", "mid", "leaf"), None),
        P(("top", "mid", "leaf"), None, None),
        P(("top", "mid", "leaf"), None, None),
        P(("top", "mid", "leaf"), None, None),
        P(("top", "mid", "leaf"), None, None),
        P(),
        P(("top", "mid", "leaf"), None, None, None),
        P(("top", "mid"), None, None, None),
        P("top", None, None, None),
        P(("top", "mid", "leaf"), None),
        P(("top", "mid"), None),
        P(("top", "mid"), None),
        P("top", None),
    )
    out_specs = P(("top", "mid", "leaf"), None)
    return jax.shard_map(body, mesh=mesh, in_specs=in_specs, out_specs=out_specs, check_vma=False)
```

```python
import jax
import jax.numpy as jnp
from jax import lax
from jax.experimental import pallas as pl
from jax.experimental.pallas import tpu as pltpu
from jax.sharding import PartitionSpec as P

damping = 0.7
MESH = pl.DeviceIdType.MESH
NY, NZ, NC = 4, 8, 8
TILES = 3
ABROAD = [(k, dy) for k in range(NC) for dy in range(NY) if k or dy]
ABROAD.sort(key=lambda p: -((0, 2, 0, 2, 1, 1, 1, 1)[p[0]] + (0, 1, 2, 1)[p[1]]))
PLACE = {0: 0, 1: 1, 7: 2, 2: 3, 6: 4, 3: 5, 5: 6, 4: 7}
PLACES = [(1, 3), (3, 4), (4, 5), (5, 8)]
STEP = {k: next(i for i, (begin, end) in enumerate(PLACES) if begin <= at < end) for k, at in PLACE.items() if k}
F32, BF16 = jnp.float32, jnp.bfloat16


def dot_nn(a, b):
    return jnp.dot(a, b, preferred_element_type=F32)


def dot_nt(a, b):
    return lax.dot_general(a, b, (((1,), (1,)), ((), ())), preferred_element_type=F32)


def dot_tn(a, b):
    return lax.dot_general(a, b, (((0,), (0,)), ((), ())), preferred_element_type=F32)


def kernel(
    lists_hbm,
    owner_hbm,
    clist_hbm,
    glist_hbm,
    rhs_hbm,
    guess_hbm,
    diag_hbm,
    prec_hbm,
    bases_hbm,
    trans_hbm,
    mid_hbm,
    coup_hbm,
    ccoup_hbm,
    gcoup_hbm,
    out_ref,
    lists_ref,
    owner_ref,
    clist_ref,
    glist_ref,
    rhs,
    guess,
    diag,
    prec,
    trans,
    mid,
    ccoup,
    gcoup,
    coup_all,
    meta_all,
    weights,
    mmat,
    emat,
    rnb,
    first,
    firsth,
    pbx,
    gmat,
    w_t,
    acc,
    coef,
    uterm_send,
    uterm_recv,
    row_recv,
    cc_all,
    far,
    loop_send,
    loop_recv,
    loop_row,
    part_send,
    part_recv,
    load_sem,
    wt_send,
    wt_recv,
    ag_send,
    ag_recv,
    rs_send,
    rs_recv,
    ys_send,
    ys_recv,
    cx_send,
    cx_recv,
    ct_send,
    ct_recv,
    lp_send,
    lp_recv,
    pt_send,
    pt_recv,
):
    top, mdl, leaf = lax.axis_index("top"), lax.axis_index("mid"), lax.axis_index("leaf")
    y, z = leaf // NZ, lax.rem(leaf, NZ)
    cluster = top * 2 + mdl
    n, cols = rhs.shape
    rank = trans.shape[1]
    piece = cols // NZ
    half = cols // 2
    strip = rank // NZ
    tile = n // TILES

    def z_peer(dz):
        return (top, mdl, y * NZ + lax.rem(z + dz, NZ))

    def y_peer(dy):
        return (top, mdl, lax.rem(y + dy, NY) * NZ + z)

    def flipped(k):
        high = lax.rem(top // 2 + k // 4, 2)
        low = lax.rem(lax.rem(top, 2) + k // 2 % 2, 2)
        return high * 2 + low, lax.rem(mdl + k % 2, 2)

    def c_peer(k, dy):
        return (*flipped(k), lax.rem(y + dy, NY) * NZ + z)

    barrier = pltpu.get_barrier_semaphore()
    for dz in (4, 3, 5, 2, 6, 1, 7):
        pl.semaphore_signal(barrier, inc=1, device_id=z_peer(dz), device_id_type=MESH)
    for dy in (2, 1, 3):
        pl.semaphore_signal(barrier, inc=1, device_id=y_peer(dy), device_id_type=MESH)
    for k in (1, 3, 4, 5, 6, 7, 2):
        pl.semaphore_signal(barrier, inc=1, device_id=c_peer(k, 0), device_id_type=MESH)

    loads = {}
    for i, (name, src, dst) in enumerate(
        (
            ("bases", bases_hbm.at[0], rnb.at[:, pl.ds(0, rank)]),
            ("trans", trans_hbm.at[0], trans),
            ("guess", guess_hbm, guess),
            ("coup", coup_hbm.at[0], coup_all.at[0]),
            ("lists", lists_hbm, lists_ref),
            ("owner", owner_hbm, owner_ref),
            ("clist", clist_hbm, clist_ref),
            ("glist", glist_hbm, glist_ref),
            ("mid", mid_hbm, mid),
            ("ccoup", ccoup_hbm.at[0], ccoup),
            ("gcoup", gcoup_hbm.at[0], gcoup),
            ("prec", prec_hbm.at[0], prec),
            ("diag", diag_hbm.at[0], diag),
            ("rhs", rhs_hbm, rhs),
        )
    ):
        loads[name] = pltpu.make_async_copy(src, dst, load_sem.at[i])
        loads[name].start()

    def send(src, dst, send_sem, recv_sem, peer):
        copy = pltpu.make_async_remote_copy(
            src_ref=src,
            dst_ref=dst,
            send_sem=send_sem,
            recv_sem=recv_sem,
            device_id=peer,
            device_id_type=MESH,
        )
        copy.start()

    def arrived(dst, send_sem, recv_sem):
        pltpu.make_async_remote_copy(
            src_ref=dst,
            dst_ref=dst,
            send_sem=send_sem,
            recv_sem=recv_sem,
            device_id=z_peer(1),
            device_id_type=MESH,
        ).wait_recv()

    def left(src, send_sem, recv_sem):
        pltpu.make_async_remote_copy(
            src_ref=src,
            dst_ref=src,
            send_sem=send_sem,
            recv_sem=recv_sem,
            device_id=z_peer(1),
            device_id_type=MESH,
        ).wait_send()

    mine = pl.ds(pl.multiple_of(z * piece, piece), piece)

    def block(r, h, k):
        return coef.at[r, pl.ds(h * half, half), pl.ds(PLACE[k] * rank, rank)]

    def pass_on(r, h, source, k, dz):
        send(block(r, h, source), block(r, h, k), ag_send.at[r], ag_recv.at[r, h, STEP[k]], z_peer(dz))

    def here(r, h, begin, end):
        blocks = coef.at[r, pl.ds(h * half, half), pl.ds(begin * rank, (end - begin) * rank)]
        arrived(blocks, ag_send.at[r], ag_recv.at[r, h, PLACES.index((begin, end))])

    def send_terms(r):
        for dz in (4, 3, 5, 2, 6, 1, 7):
            there = lax.rem(z + dz, NZ)
            send(
                uterm_send.at[r, pl.ds(pl.multiple_of(there * piece, piece), piece)],
                uterm_recv.at[r, NZ - dz],
                rs_send.at[r],
                rs_recv.at[r],
                z_peer(dz),
            )

    def send_coefs(r):
        for dz in (2, 6, 1, 7):
            for h in range(2):
                pass_on(r, h, 0, NZ - dz, dz)

    def send_loop():
        loop_send[...] = gmat[rank:, rank:]
        for dz in (4, 3, 5, 2, 6, 1, 7):
            there = pl.ds(pl.multiple_of(lax.rem(z + dz, NZ) * strip, strip), strip)
            send(loop_send.at[there], loop_recv.at[NZ - dz], lp_send.at[0], lp_recv.at[0], z_peer(dz))

    def pass_loop():
        arrived(loop_recv.at[pl.ds(1, NZ - 1)], lp_send.at[0], lp_recv.at[0])
        own = pl.ds(pl.multiple_of(z * strip, strip), strip)
        total = loop_send[own].astype(F32)
        for k in range(1, NZ):
            total = total + loop_recv[k].astype(F32)
        loop_row[own] = total.astype(BF16)
        for dz in (4, 3, 5, 2, 6, 1, 7):
            send(loop_row.at[own], loop_row.at[own], lp_send.at[1], lp_recv.at[1], z_peer(dz))

    def relay(r, h):
        here(r, h, 4, 5)
        if h == 0:
            pass_on(r, h, 6, 4, 2)
        pass_on(r, h, 6, 5, 1)
        here(r, h, 3, 4)
        if h == 1:
            pass_on(r, h, 2, 4, 6)
        pass_on(r, h, 2, 3, 7)

    def row_sum(r):
        arrived(uterm_recv.at[r, pl.ds(1, NZ - 1)], rs_send.at[r], rs_recv.at[r])
        total = uterm_send[r, mine].astype(F32)
        for k in range(1, NZ):
            total = total + uterm_recv[r, k].astype(F32)
        if r == 1:
            arrived(loop_row.at[pl.ds(0, rank - strip)], lp_send.at[1], lp_recv.at[1])
            total = total - damping * dot_nt(far[0, mine, rank:], loop_row[...])
        if r == 0:
            cc_all[0, :, 0:rank] = total.astype(BF16)
            for k in (1, 3, 4, 5, 6, 7, 2):
                there = cc_all.at[0, :, pl.ds(k * rank, rank)]
                send(cc_all.at[0, :, pl.ds(0, rank)], there, cx_send, cx_recv, c_peer(k, 0))
        else:
            row_recv[1, 0] = total.astype(BF16)
            for k, dy in ABROAD:
                there = row_recv.at[1, k * NY + (NY - dy) % NY]
                send(row_recv.at[1, 0], there, ys_send.at[1], ys_recv.at[1], c_peer(k, dy))

    def column_sum(r, k):
        total = row_recv[r, k * NY].astype(F32)
        for dy in range(1, NY):
            total = total + row_recv[r, k * NY + dy].astype(F32)
        return total

    def pass_sum():
        arrived(cc_all.at[0, :, pl.ds(rank, (NC - 1) * rank)], cx_send, cx_recv)
        row_recv[0, 0] = dot_nt(cc_all[0], mmat[...]).astype(BF16)
        for dy in (2, 1, 3):
            send(row_recv.at[0, 0], row_recv.at[0, NY - dy], ys_send.at[0], ys_recv.at[0], y_peer(dy))

    def cluster_total(r):
        if r == 0:
            arrived(row_recv.at[0, pl.ds(1, NY - 1)], ys_send.at[0], ys_recv.at[0])
            total = column_sum(0, 0)
        else:
            arrived(row_recv.at[1, pl.ds(1, NC * NY - 1)], ys_send.at[1], ys_recv.at[1])
            for k in range(NC):
                cc_all[1, :, k * rank : (k + 1) * rank] = column_sum(1, k).astype(BF16)
            total = dot_nt(cc_all[1], mmat[...])
        far[r, mine, rank:] = total.astype(BF16)
        there = far.at[r, mine, pl.ds(rank, rank)]
        for dz in (4, 3, 5, 2, 6, 1, 7):
            send(there, there, ct_send.at[r], ct_recv.at[r], z_peer(dz))

    def early_sums(r):
        for h in range(2):
            here(r, h, 1, 3)
        acc[...] = dot_nt(coef[r, :, 0 : 5 * rank], weights[:, 0 : 5 * rank])

    def late_sums(r, h):
        here(r, h, 5, 8)
        rows = slice(h * half, (h + 1) * half)
        if r == 0:
            here(r, h, 1, 3)
            value = dot_nt(coef[r, rows], weights[...])
        else:
            value = acc[rows] + dot_nt(coef[r, rows, 5 * rank :], weights[:, 5 * rank :])
        acc[rows, 0:rank] = value[:, 0:rank]
        for j in (2, 1, 3):
            part_send[r, j, rows] = value[:, j * rank : (j + 1) * rank].astype(BF16)
        for j in (2, 1, 3):
            send(
                part_send.at[r, j, pl.ds(h * half, half)],
                part_recv.at[r, h, NY - j],
                pt_send.at[r],
                pt_recv.at[r, h],
                y_peer(j),
            )

    def leaf_sum(r):
        for h in range(2):
            arrived(part_recv.at[r, h, pl.ds(1, NY - 1)], pt_send.at[r], pt_recv.at[r, h])
        for h in range(2):
            at = slice(h * half, (h + 1) * half)
            total = acc[at, 0:rank]
            for k in range(1, NY):
                total = total + part_recv[r, h, k].astype(F32)
            far[r, at, 0:rank] = total.astype(BF16)

    def gather_total(r):
        arrived(far.at[r, pl.ds(0, cols - piece), pl.ds(rank, rank)], ct_send.at[r], ct_recv.at[r])

    def all_left(r):
        left(uterm_send.at[r, pl.ds(0, cols - piece)], rs_send.at[r], rs_recv.at[r])
        left(coef.at[r, :, pl.ds(0, 7 * rank)], ag_send.at[r], ag_recv.at[r, 0, 0])
        if r == 0:
            left(row_recv.at[r, pl.ds(1, NY - 1)], ys_send.at[r], ys_recv.at[r])
            left(cc_all.at[r, :, pl.ds(rank, (NC - 1) * rank)], cx_send, cx_recv)
        else:
            left(row_recv.at[r, pl.ds(1, NC * NY - 1)], ys_send.at[r], ys_recv.at[r])
        left(far.at[r, pl.ds(0, cols - piece), pl.ds(rank, rank)], ct_send.at[r], ct_recv.at[r])
        left(part_send.at[r, pl.ds(1, NY - 1)], pt_send.at[r], pt_recv.at[r, 0])

    def tiles(step, begin=0, end=TILES):
        def run(i, carry):
            step(pl.ds(pl.multiple_of(i * tile, tile), tile))
            return carry

        lax.fori_loop(begin, end, run, 0)

    loads["bases"].wait()
    loads["trans"].wait()
    rnb[:, rank : 2 * rank] = dot_nn(rnb[:, 0:rank], trans[...]).astype(BF16)
    bases = rnb.at[:, pl.ds(0, 2 * rank)]
    loads["guess"].wait()
    both = dot_tn(guess[...], bases[...]).astype(BF16)
    uterm_send[0] = both[:, rank:]
    coef[0, :, 0:rank] = both[:, 0:rank]
    pl.semaphore_wait(barrier, NZ + NY + NC - 3)
    send_terms(0)
    send_coefs(0)

    loads["coup"].wait()
    loads["lists"].wait()
    loads["owner"].wait()
    rows = lax.broadcasted_iota(jnp.int32, (8, rank), 0)
    meta = jnp.zeros((8, rank), jnp.int32)
    for k in range(4):
        meta = jnp.where(rows == k, owner_ref[0, lists_ref[0, k]], meta)
    meta_all[0] = meta
    for dy in (2, 1, 3):
        send(coup_all.at[0], coup_all.at[NY - dy], wt_send.at[1], wt_recv.at[1], y_peer(dy))
        send(meta_all.at[0], meta_all.at[NY - dy], wt_send.at[0], wt_recv.at[0], y_peer(dy))

    for name in ("mid", "gcoup", "ccoup", "clist", "glist"):
        loads[name].wait()
    for k in range(2):
        emat[k] = dot_nn(mid[cluster], gcoup[k])

    def compose(k, carry):
        there, also = flipped(k)
        other = there * 2 + also
        pick = jnp.zeros((rank, rank), F32)
        for i in range(2):
            pick = pick + jnp.where(glist_ref[0, i] == there, 1.0, 0.0) * emat[i]
        value = dot_nt(pick.astype(BF16), mid[other])
        for i in range(3):
            value = value + jnp.where(clist_ref[0, i] == other, 1.0, 0.0) * ccoup[i].astype(F32)
        mmat[:, pl.ds(pl.multiple_of(k * rank, rank), rank)] = value.astype(BF16)
        return carry

    lax.fori_loop(0, NC, compose, 0)

    loads["prec"].wait()

    def smooth_bases(at):
        pbx[at] = dot_nn(prec[at], bases[...]).astype(BF16)

    tiles(smooth_bases)
    gmat[...] = dot_tn(bases[...], pbx[...]).astype(BF16)
    send_loop()

    row_sum(0)
    relay(0, 0)
    relay(0, 1)

    loads["rhs"].wait()
    loads["diag"].wait()

    def near(at):
        rnb[at, 2 * rank :] = (rhs[at].astype(F32) - dot_nn(diag[at], guess[...])).astype(BF16)

    tiles(near, 0, 2)

    arrived(meta_all.at[pl.ds(1, NY - 1)], wt_send.at[0], wt_recv.at[0])
    arrived(coup_all.at[pl.ds(1, NY - 1)], wt_send.at[1], wt_recv.at[1])

    def place(p, carry):
        away = ((p + 1) // 2) * (2 * lax.rem(p, 2) - 1)
        slot = y * NZ + lax.rem(z + away + NZ, NZ)
        for j in range(NY):
            hit = jnp.where(meta_all[j] == slot, 1.0, 0.0).astype(BF16)
            value = hit[0:1] * coup_all[j, 0]
            for i in range(1, 4):
                value = value + hit[i : i + 1] * coup_all[j, i]
            weights[j * rank : (j + 1) * rank, pl.ds(pl.multiple_of(p * rank, rank), rank)] = value
        return carry

    lax.fori_loop(0, NZ, place, 0)
    pass_sum()
    late_sums(0, 0)
    late_sums(0, 1)
    tiles(near, 2, 3)
    cluster_total(0)
    pass_loop()

    def smooth(at):
        base = guess[at].astype(F32) + damping * dot_nn(prec[at], rnb[:, 2 * rank :])
        first[at] = base
        firsth[at] = base.astype(BF16)

    tiles(smooth)
    w_t[...] = dot_tn(firsth[...], bases[...])
    leaf_sum(0)
    uterm_send[1] = (w_t[:, rank:] - damping * dot_nt(far[0, :, 0:rank], gmat[rank:, 0:rank])).astype(BF16)
    send_terms(1)
    gather_total(0)
    coef[1, :, 0:rank] = (w_t[:, 0:rank] - damping * dot_nt(far[0], gmat[0:rank])).astype(BF16)
    send_coefs(1)

    def correct(at):
        value = first[at] - damping * dot_nt(pbx[at], far[0])
        first[at] = value
        firsth[at] = value.astype(BF16)

    correct(slice(0, n))

    def near_again(at):
        rnb[at, 2 * rank :] = (rhs[at].astype(F32) - dot_nn(diag[at], firsth[...])).astype(BF16)

    tiles(near_again)
    row_sum(1)
    relay(1, 0)
    relay(1, 1)

    def smooth_again(at):
        first[at] = first[at] + damping * dot_nn(prec[at], rnb[:, 2 * rank :])

    tiles(smooth_again)
    early_sums(1)
    late_sums(1, 0)
    late_sums(1, 1)
    cluster_total(1)
    all_left(0)
    left(loop_send.at[pl.ds(0, rank - strip)], lp_send.at[0], lp_recv.at[0])
    left(loop_row.at[pl.ds(0, rank - strip)], lp_send.at[1], lp_recv.at[1])
    left(meta_all.at[pl.ds(1, NY - 1)], wt_send.at[0], wt_recv.at[0])
    left(coup_all.at[pl.ds(1, NY - 1)], wt_send.at[1], wt_recv.at[1])
    leaf_sum(1)
    gather_total(1)

    def finish(at):
        out_ref[at] = (first[at] - damping * dot_nt(pbx[at], far[1])).astype(BF16)

    finish(slice(0, n))
    all_left(1)


def body(
    rhs,
    guess,
    diag_blocks,
    precond,
    bases,
    leaf_to_middle_transfer,
    mid_transfer,
    leaf_coupling,
    cluster_coupling,
    group_coupling,
    leaf_lists,
    owner,
    cluster_lists,
    group_lists,
):
    n, cols = rhs.shape
    rank = bases.shape[2]
    piece = cols // NZ
    hbm = pl.BlockSpec(memory_space=pltpu.HBM)
    dma = pltpu.SemaphoreType.DMA
    return pl.pallas_call(
        kernel,
        out_shape=pltpu.VMEM((n, cols), BF16),
        in_specs=[hbm] * 14,
        out_specs=pl.BlockSpec(memory_space=pltpu.VMEM),
        scratch_shapes=[
            pltpu.SMEM(leaf_lists.shape, jnp.int32),
            pltpu.SMEM(owner.shape, jnp.int32),
            pltpu.SMEM(cluster_lists.shape, jnp.int32),
            pltpu.SMEM(group_lists.shape, jnp.int32),
            pltpu.VMEM((n, cols), BF16),
            pltpu.VMEM((n, cols), BF16),
            pltpu.VMEM((n, n), BF16),
            pltpu.VMEM((n, n), BF16),
            pltpu.VMEM((rank, rank), BF16),
            pltpu.VMEM((NC, rank, rank), BF16),
            pltpu.VMEM((3, rank, rank), BF16),
            pltpu.VMEM((2, rank, rank), BF16),
            pltpu.VMEM((NY, 4, rank, rank), BF16),
            pltpu.VMEM((NY, 8, rank), jnp.int32),
            pltpu.VMEM((NY * rank, NZ * rank), BF16),
            pltpu.VMEM((rank, NC * rank), BF16),
            pltpu.VMEM((2, rank, rank), F32),
            pltpu.VMEM((n, cols + 2 * rank), BF16),
            pltpu.VMEM((n, cols), F32),
            pltpu.VMEM((n, cols), BF16),
            pltpu.VMEM((n, 2 * rank), BF16),
            pltpu.VMEM((2 * rank, 2 * rank), BF16),
            pltpu.VMEM((cols, 2 * rank), F32),
            pltpu.VMEM((cols, NY * rank), F32),
            pltpu.VMEM((2, cols, NZ * rank), BF16),
            pltpu.VMEM((2, cols, rank), BF16),
            pltpu.VMEM((2, NZ, piece, rank), BF16),
            pltpu.VMEM((2, NC * NY, piece, rank), BF16),
            pltpu.VMEM((2, piece, NC * rank), BF16),
            pltpu.VMEM((2, cols, 2 * rank), BF16),
            pltpu.VMEM((rank, rank), BF16),
            pltpu.VMEM((NZ, rank // NZ, rank), BF16),
            pltpu.VMEM((rank, rank), BF16),
            pltpu.VMEM((2, NY, cols, rank), BF16),
            pltpu.VMEM((2, 2, NY, cols // 2, rank), BF16),
            dma((14,)),
            dma((2,)),
            dma((2,)),
            dma((2,)),
            dma((2, 2, len(PLACES))),
            dma((2,)),
            dma((2,)),
            dma((2,)),
            dma((2,)),
            dma,
            dma,
            dma((2,)),
            dma((2,)),
            dma((2,)),
            dma((2,)),
            dma((2,)),
            dma((2, 2)),
        ],
        compiler_params=pltpu.CompilerParams(
            collective_id=0, has_side_effects=True, vmem_limit_bytes=67043328 - n * cols * 2
        ),
    )(
        leaf_lists,
        owner,
        cluster_lists,
        group_lists,
        rhs,
        guess,
        diag_blocks,
        precond,
        bases,
        leaf_to_middle_transfer,
        mid_transfer,
        leaf_coupling,
        cluster_coupling,
        group_coupling,
    )


def solution(mesh):
    in_specs = (
        P(("top", "mid", "leaf"), None),
        P(("top", "mid", "leaf"), None),
        P(("top", "mid", "leaf"), None, None),
        P(("top", "mid", "leaf"), None, None),
        P(("top", "mid", "leaf"), None, None),
        P(("top", "mid", "leaf"), None, None),
        P(),
        P(("top", "mid", "leaf"), None, None, None),
        P(("top", "mid"), None, None, None),
        P("top", None, None, None),
        P(("top", "mid", "leaf"), None),
        P(("top", "mid"), None),
        P(("top", "mid"), None),
        P("top", None),
    )
    out_specs = P(("top", "mid", "leaf"), None)
    return jax.shard_map(body, mesh=mesh, in_specs=in_specs, out_specs=out_specs, check_vma=False)
```

```python
import jax
import jax.numpy as jnp
from jax import lax
from jax.experimental import pallas as pl
from jax.experimental.pallas import tpu as pltpu
from jax.sharding import PartitionSpec as P

damping = 0.7
MESH = pl.DeviceIdType.MESH
NY, NZ, NC = 4, 8, 8
TILES = 3
ABROAD = [(k, dy) for k in range(NC) for dy in range(NY) if k or dy]
ABROAD.sort(key=lambda p: -((0, 2, 0, 2, 1, 1, 1, 1)[p[0]] + (0, 1, 2, 1)[p[1]]))
PLACE = {0: 0, 1: 1, 7: 2, 2: 3, 6: 4, 3: 5, 5: 6, 4: 7}
PLACES = [(1, 3), (3, 4), (4, 5), (5, 8)]
STEP = {k: next(i for i, (begin, end) in enumerate(PLACES) if begin <= at < end) for k, at in PLACE.items() if k}
F32, BF16 = jnp.float32, jnp.bfloat16


def dot_nn(a, b):
    return jnp.dot(a, b, preferred_element_type=F32)


def dot_nt(a, b):
    return lax.dot_general(a, b, (((1,), (1,)), ((), ())), preferred_element_type=F32)


def dot_tn(a, b):
    return lax.dot_general(a, b, (((0,), (0,)), ((), ())), preferred_element_type=F32)


def kernel(
    lists_hbm,
    owner_hbm,
    clist_hbm,
    glist_hbm,
    rhs_hbm,
    guess_hbm,
    diag_hbm,
    prec_hbm,
    bases_hbm,
    trans_hbm,
    mid_hbm,
    coup_hbm,
    ccoup_hbm,
    gcoup_hbm,
    out_ref,
    lists_ref,
    owner_ref,
    clist_ref,
    glist_ref,
    rhs,
    guess,
    diag,
    prec,
    trans,
    mid,
    ccoup,
    gcoup,
    coup_all,
    meta_all,
    weights,
    mmat,
    emat,
    rnb,
    first,
    firsth,
    pbx,
    gmat,
    w_t,
    acc,
    coef,
    uterm_send,
    uterm_recv,
    row_recv,
    cc_all,
    far,
    loop_send,
    loop_recv,
    loop_row,
    part_send,
    part_recv,
    load_sem,
    wt_send,
    wt_recv,
    ag_send,
    ag_recv,
    rs_send,
    rs_recv,
    ys_send,
    ys_recv,
    cx_send,
    cx_recv,
    ct_send,
    ct_recv,
    lp_send,
    lp_recv,
    pt_send,
    pt_recv,
):
    top, mdl, leaf = lax.axis_index("top"), lax.axis_index("mid"), lax.axis_index("leaf")
    y, z = leaf // NZ, lax.rem(leaf, NZ)
    cluster = top * 2 + mdl
    n, cols = rhs.shape
    rank = trans.shape[1]
    piece = cols // NZ
    half = cols // 2
    strip = rank // NZ
    tile = n // TILES

    def z_peer(dz):
        return (top, mdl, y * NZ + lax.rem(z + dz, NZ))

    def y_peer(dy):
        return (top, mdl, lax.rem(y + dy, NY) * NZ + z)

    def flipped(k):
        high = lax.rem(top // 2 + k // 4, 2)
        low = lax.rem(lax.rem(top, 2) + k // 2 % 2, 2)
        return high * 2 + low, lax.rem(mdl + k % 2, 2)

    def c_peer(k, dy):
        return (*flipped(k), lax.rem(y + dy, NY) * NZ + z)

    barrier = pltpu.get_barrier_semaphore()
    for dz in (4, 3, 5, 2, 6, 1, 7):
        pl.semaphore_signal(barrier, inc=1, device_id=z_peer(dz), device_id_type=MESH)
    for dy in (2, 1, 3):
        pl.semaphore_signal(barrier, inc=1, device_id=y_peer(dy), device_id_type=MESH)
    for k in (1, 3, 4, 5, 6, 7, 2):
        pl.semaphore_signal(barrier, inc=1, device_id=c_peer(k, 0), device_id_type=MESH)

    loads = {}
    for i, (name, src, dst) in enumerate(
        (
            ("bases", bases_hbm.at[0], rnb.at[:, pl.ds(0, rank)]),
            ("trans", trans_hbm.at[0], trans),
            ("guess", guess_hbm, guess),
            ("coup", coup_hbm.at[0], coup_all.at[0]),
            ("lists", lists_hbm, lists_ref),
            ("owner", owner_hbm, owner_ref),
            ("clist", clist_hbm, clist_ref),
            ("glist", glist_hbm, glist_ref),
            ("mid", mid_hbm, mid),
            ("ccoup", ccoup_hbm.at[0], ccoup),
            ("gcoup", gcoup_hbm.at[0], gcoup),
            ("prec", prec_hbm.at[0], prec),
            ("diag", diag_hbm.at[0], diag),
            ("rhs", rhs_hbm, rhs),
        )
    ):
        loads[name] = pltpu.make_async_copy(src, dst, load_sem.at[i])
        loads[name].start()

    def send(src, dst, send_sem, recv_sem, peer):
        copy = pltpu.make_async_remote_copy(
            src_ref=src,
            dst_ref=dst,
            send_sem=send_sem,
            recv_sem=recv_sem,
            device_id=peer,
            device_id_type=MESH,
        )
        copy.start()

    def arrived(dst, send_sem, recv_sem):
        pltpu.make_async_remote_copy(
            src_ref=dst,
            dst_ref=dst,
            send_sem=send_sem,
            recv_sem=recv_sem,
            device_id=z_peer(1),
            device_id_type=MESH,
        ).wait_recv()

    def left(src, send_sem, recv_sem):
        pltpu.make_async_remote_copy(
            src_ref=src,
            dst_ref=src,
            send_sem=send_sem,
            recv_sem=recv_sem,
            device_id=z_peer(1),
            device_id_type=MESH,
        ).wait_send()

    mine = pl.ds(pl.multiple_of(z * piece, piece), piece)

    def block(r, h, k):
        return coef.at[r, pl.ds(h * half, half), pl.ds(PLACE[k] * rank, rank)]

    def pass_on(r, h, source, k, dz):
        send(block(r, h, source), block(r, h, k), ag_send.at[r], ag_recv.at[r, h, STEP[k]], z_peer(dz))

    def here(r, h, begin, end):
        blocks = coef.at[r, pl.ds(h * half, half), pl.ds(begin * rank, (end - begin) * rank)]
        arrived(blocks, ag_send.at[r], ag_recv.at[r, h, PLACES.index((begin, end))])

    def send_terms(r):
        for dz in (4, 3, 5, 2, 6, 1, 7):
            there = lax.rem(z + dz, NZ)
            send(
                uterm_send.at[r, pl.ds(pl.multiple_of(there * piece, piece), piece)],
                uterm_recv.at[r, NZ - dz],
                rs_send.at[r],
                rs_recv.at[r],
                z_peer(dz),
            )

    def send_coefs(r):
        for dz in (2, 6, 1, 7):
            for h in range(2):
                pass_on(r, h, 0, NZ - dz, dz)

    def send_loop():
        loop_send[...] = gmat[rank:, rank:]
        for dz in (4, 3, 5, 2, 6, 1, 7):
            there = pl.ds(pl.multiple_of(lax.rem(z + dz, NZ) * strip, strip), strip)
            send(loop_send.at[there], loop_recv.at[NZ - dz], lp_send.at[0], lp_recv.at[0], z_peer(dz))

    def pass_loop():
        arrived(loop_recv.at[pl.ds(1, NZ - 1)], lp_send.at[0], lp_recv.at[0])
        own = pl.ds(pl.multiple_of(z * strip, strip), strip)
        total = loop_send[own].astype(F32)
        for k in range(1, NZ):
            total = total + loop_recv[k].astype(F32)
        loop_row[own] = total.astype(BF16)
        for dz in (4, 3, 5, 2, 6, 1, 7):
            send(loop_row.at[own], loop_row.at[own], lp_send.at[1], lp_recv.at[1], z_peer(dz))

    def relay(r, h):
        here(r, h, 4, 5)
        if h == 0:
            pass_on(r, h, 6, 4, 2)
        pass_on(r, h, 6, 5, 1)
        here(r, h, 3, 4)
        if h == 1:
            pass_on(r, h, 2, 4, 6)
        pass_on(r, h, 2, 3, 7)

    def row_sum(r):
        arrived(uterm_recv.at[r, pl.ds(1, NZ - 1)], rs_send.at[r], rs_recv.at[r])
        total = uterm_send[r, mine].astype(F32)
        for k in range(1, NZ):
            total = total + uterm_recv[r, k].astype(F32)
        if r == 1:
            arrived(loop_row.at[pl.ds(0, rank - strip)], lp_send.at[1], lp_recv.at[1])
            total = total - damping * dot_nt(far[0, mine, rank:], loop_row[...])
        if r == 0:
            cc_all[0, :, 0:rank] = total.astype(BF16)
            for k in (1, 3, 4, 5, 6, 7, 2):
                there = cc_all.at[0, :, pl.ds(k * rank, rank)]
                send(cc_all.at[0, :, pl.ds(0, rank)], there, cx_send, cx_recv, c_peer(k, 0))
        else:
            row_recv[1, 0] = total.astype(BF16)
            for k, dy in ABROAD:
                there = row_recv.at[1, k * NY + (NY - dy) % NY]
                send(row_recv.at[1, 0], there, ys_send.at[1], ys_recv.at[1], c_peer(k, dy))

    def column_sum(r, k):
        total = row_recv[r, k * NY].astype(F32)
        for dy in range(1, NY):
            total = total + row_recv[r, k * NY + dy].astype(F32)
        return total

    def pass_sum():
        arrived(cc_all.at[0, :, pl.ds(rank, (NC - 1) * rank)], cx_send, cx_recv)
        row_recv[0, 0] = dot_nt(cc_all[0], mmat[...]).astype(BF16)
        for dy in (2, 1, 3):
            send(row_recv.at[0, 0], row_recv.at[0, NY - dy], ys_send.at[0], ys_recv.at[0], y_peer(dy))

    def cluster_total(r):
        if r == 0:
            arrived(row_recv.at[0, pl.ds(1, NY - 1)], ys_send.at[0], ys_recv.at[0])
            total = column_sum(0, 0)
        else:
            arrived(row_recv.at[1, pl.ds(1, NC * NY - 1)], ys_send.at[1], ys_recv.at[1])
            for k in range(NC):
                cc_all[1, :, k * rank : (k + 1) * rank] = column_sum(1, k).astype(BF16)
            total = dot_nt(cc_all[1], mmat[...])
        far[r, mine, rank:] = total.astype(BF16)
        there = far.at[r, mine, pl.ds(rank, rank)]
        for dz in (4, 3, 5, 2, 6, 1, 7):
            send(there, there, ct_send.at[r], ct_recv.at[r], z_peer(dz))

    def early_sums(r):
        for h in range(2):
            here(r, h, 1, 3)
        acc[...] = dot_nt(coef[r, :, 0 : 5 * rank], weights[:, 0 : 5 * rank])

    def late_sums(r, h):
        here(r, h, 5, 8)
        rows = slice(h * half, (h + 1) * half)
        if r == 0:
            here(r, h, 1, 3)
            value = dot_nt(coef[r, rows], weights[...])
        else:
            value = acc[rows] + dot_nt(coef[r, rows, 5 * rank :], weights[:, 5 * rank :])
        acc[rows, 0:rank] = value[:, 0:rank]
        for j in (2, 1, 3):
            part_send[r, j, rows] = value[:, j * rank : (j + 1) * rank].astype(BF16)
        for j in (2, 1, 3):
            send(
                part_send.at[r, j, pl.ds(h * half, half)],
                part_recv.at[r, h, NY - j],
                pt_send.at[r],
                pt_recv.at[r, h],
                y_peer(j),
            )

    def leaf_sum(r):
        for h in range(2):
            arrived(part_recv.at[r, h, pl.ds(1, NY - 1)], pt_send.at[r], pt_recv.at[r, h])
        for h in range(2):
            at = slice(h * half, (h + 1) * half)
            total = acc[at, 0:rank]
            for k in range(1, NY):
                total = total + part_recv[r, h, k].astype(F32)
            far[r, at, 0:rank] = total.astype(BF16)

    def gather_total(r):
        arrived(far.at[r, pl.ds(0, cols - piece), pl.ds(rank, rank)], ct_send.at[r], ct_recv.at[r])

    def all_left(r):
        left(uterm_send.at[r, pl.ds(0, cols - piece)], rs_send.at[r], rs_recv.at[r])
        left(coef.at[r, :, pl.ds(0, 7 * rank)], ag_send.at[r], ag_recv.at[r, 0, 0])
        if r == 0:
            left(row_recv.at[r, pl.ds(1, NY - 1)], ys_send.at[r], ys_recv.at[r])
            left(cc_all.at[r, :, pl.ds(rank, (NC - 1) * rank)], cx_send, cx_recv)
        else:
            left(row_recv.at[r, pl.ds(1, NC * NY - 1)], ys_send.at[r], ys_recv.at[r])
        left(far.at[r, pl.ds(0, cols - piece), pl.ds(rank, rank)], ct_send.at[r], ct_recv.at[r])
        left(part_send.at[r, pl.ds(1, NY - 1)], pt_send.at[r], pt_recv.at[r, 0])

    def tiles(step, begin=0, end=TILES):
        def run(i, carry):
            step(pl.ds(pl.multiple_of(i * tile, tile), tile))
            return carry

        lax.fori_loop(begin, end, run, 0)

    loads["bases"].wait()
    loads["trans"].wait()
    rnb[:, rank : 2 * rank] = dot_nn(rnb[:, 0:rank], trans[...]).astype(BF16)
    bases = rnb.at[:, pl.ds(0, 2 * rank)]
    loads["guess"].wait()
    both = dot_tn(guess[...], bases[...]).astype(BF16)
    uterm_send[0] = both[:, rank:]
    coef[0, :, 0:rank] = both[:, 0:rank]
    pl.semaphore_wait(barrier, NZ + NY + NC - 3)
    send_terms(0)
    send_coefs(0)

    loads["coup"].wait()
    loads["lists"].wait()
    loads["owner"].wait()
    rows = lax.broadcasted_iota(jnp.int32, (8, rank), 0)
    meta = jnp.zeros((8, rank), jnp.int32)
    for k in range(4):
        meta = jnp.where(rows == k, owner_ref[0, lists_ref[0, k]], meta)
    meta_all[0] = meta
    for dy in (2, 1, 3):
        send(coup_all.at[0], coup_all.at[NY - dy], wt_send.at[1], wt_recv.at[1], y_peer(dy))
        send(meta_all.at[0], meta_all.at[NY - dy], wt_send.at[0], wt_recv.at[0], y_peer(dy))

    for name in ("mid", "gcoup", "ccoup", "clist", "glist"):
        loads[name].wait()
    for k in range(2):
        emat[k] = dot_nn(mid[cluster], gcoup[k])

    def compose(k, carry):
        there, also = flipped(k)
        other = there * 2 + also
        pick = jnp.zeros((rank, rank), F32)
        for i in range(2):
            pick = pick + jnp.where(glist_ref[0, i] == there, 1.0, 0.0) * emat[i]
        value = dot_nt(pick.astype(BF16), mid[other])
        for i in range(3):
            value = value + jnp.where(clist_ref[0, i] == other, 1.0, 0.0) * ccoup[i].astype(F32)
        mmat[:, pl.ds(pl.multiple_of(k * rank, rank), rank)] = value.astype(BF16)
        return carry

    lax.fori_loop(0, NC, compose, 0)

    loads["prec"].wait()

    def smooth_bases(at):
        pbx[at] = dot_nn(prec[at], bases[...]).astype(BF16)

    tiles(smooth_bases)
    gmat[...] = dot_tn(bases[...], pbx[...]).astype(BF16)

    row_sum(0)
    relay(0, 0)
    relay(0, 1)
    send_loop()

    loads["rhs"].wait()
    loads["diag"].wait()

    def near(at):
        rnb[at, 2 * rank :] = (rhs[at].astype(F32) - dot_nn(diag[at], guess[...])).astype(BF16)

    tiles(near, 0, 2)

    arrived(meta_all.at[pl.ds(1, NY - 1)], wt_send.at[0], wt_recv.at[0])
    arrived(coup_all.at[pl.ds(1, NY - 1)], wt_send.at[1], wt_recv.at[1])

    def place(p, carry):
        away = ((p + 1) // 2) * (2 * lax.rem(p, 2) - 1)
        slot = y * NZ + lax.rem(z + away + NZ, NZ)
        for j in range(NY):
            hit = jnp.where(meta_all[j] == slot, 1.0, 0.0).astype(BF16)
            value = hit[0:1] * coup_all[j, 0]
            for i in range(1, 4):
                value = value + hit[i : i + 1] * coup_all[j, i]
            weights[j * rank : (j + 1) * rank, pl.ds(pl.multiple_of(p * rank, rank), rank)] = value
        return carry

    lax.fori_loop(0, NZ, place, 0)
    pass_sum()
    tiles(near, 2, 3)
    late_sums(0, 0)
    late_sums(0, 1)
    cluster_total(0)
    pass_loop()

    def smooth(at):
        base = guess[at].astype(F32) + damping * dot_nn(prec[at], rnb[:, 2 * rank :])
        first[at] = base
        firsth[at] = base.astype(BF16)

    tiles(smooth)
    w_t[...] = dot_tn(firsth[...], bases[...])
    leaf_sum(0)
    uterm_send[1] = (w_t[:, rank:] - damping * dot_nt(far[0, :, 0:rank], gmat[rank:, 0:rank])).astype(BF16)
    send_terms(1)
    gather_total(0)
    coef[1, :, 0:rank] = (w_t[:, 0:rank] - damping * dot_nt(far[0], gmat[0:rank])).astype(BF16)
    send_coefs(1)

    def correct(at):
        value = first[at] - damping * dot_nt(pbx[at], far[0])
        first[at] = value
        firsth[at] = value.astype(BF16)

    correct(slice(0, n))

    def near_again(at):
        rnb[at, 2 * rank :] = (rhs[at].astype(F32) - dot_nn(diag[at], firsth[...])).astype(BF16)

    tiles(near_again)
    row_sum(1)
    relay(1, 0)
    relay(1, 1)

    def smooth_again(at):
        first[at] = first[at] + damping * dot_nn(prec[at], rnb[:, 2 * rank :])

    tiles(smooth_again)
    early_sums(1)
    late_sums(1, 0)
    late_sums(1, 1)
    cluster_total(1)
    all_left(0)
    left(loop_send.at[pl.ds(0, rank - strip)], lp_send.at[0], lp_recv.at[0])
    left(loop_row.at[pl.ds(0, rank - strip)], lp_send.at[1], lp_recv.at[1])
    left(meta_all.at[pl.ds(1, NY - 1)], wt_send.at[0], wt_recv.at[0])
    left(coup_all.at[pl.ds(1, NY - 1)], wt_send.at[1], wt_recv.at[1])
    leaf_sum(1)
    gather_total(1)

    def finish(at):
        out_ref[at] = (first[at] - damping * dot_nt(pbx[at], far[1])).astype(BF16)

    finish(slice(0, n))
    all_left(1)


def body(
    rhs,
    guess,
    diag_blocks,
    precond,
    bases,
    leaf_to_middle_transfer,
    mid_transfer,
    leaf_coupling,
    cluster_coupling,
    group_coupling,
    leaf_lists,
    owner,
    cluster_lists,
    group_lists,
):
    n, cols = rhs.shape
    rank = bases.shape[2]
    piece = cols // NZ
    hbm = pl.BlockSpec(memory_space=pltpu.HBM)
    dma = pltpu.SemaphoreType.DMA
    return pl.pallas_call(
        kernel,
        out_shape=pltpu.VMEM((n, cols), BF16),
        in_specs=[hbm] * 14,
        out_specs=pl.BlockSpec(memory_space=pltpu.VMEM),
        scratch_shapes=[
            pltpu.SMEM(leaf_lists.shape, jnp.int32),
            pltpu.SMEM(owner.shape, jnp.int32),
            pltpu.SMEM(cluster_lists.shape, jnp.int32),
            pltpu.SMEM(group_lists.shape, jnp.int32),
            pltpu.VMEM((n, cols), BF16),
            pltpu.VMEM((n, cols), BF16),
            pltpu.VMEM((n, n), BF16),
            pltpu.VMEM((n, n), BF16),
            pltpu.VMEM((rank, rank), BF16),
            pltpu.VMEM((NC, rank, rank), BF16),
            pltpu.VMEM((3, rank, rank), BF16),
            pltpu.VMEM((2, rank, rank), BF16),
            pltpu.VMEM((NY, 4, rank, rank), BF16),
            pltpu.VMEM((NY, 8, rank), jnp.int32),
            pltpu.VMEM((NY * rank, NZ * rank), BF16),
            pltpu.VMEM((rank, NC * rank), BF16),
            pltpu.VMEM((2, rank, rank), F32),
            pltpu.VMEM((n, cols + 2 * rank), BF16),
            pltpu.VMEM((n, cols), F32),
            pltpu.VMEM((n, cols), BF16),
            pltpu.VMEM((n, 2 * rank), BF16),
            pltpu.VMEM((2 * rank, 2 * rank), BF16),
            pltpu.VMEM((cols, 2 * rank), F32),
            pltpu.VMEM((cols, NY * rank), F32),
            pltpu.VMEM((2, cols, NZ * rank), BF16),
            pltpu.VMEM((2, cols, rank), BF16),
            pltpu.VMEM((2, NZ, piece, rank), BF16),
            pltpu.VMEM((2, NC * NY, piece, rank), BF16),
            pltpu.VMEM((2, piece, NC * rank), BF16),
            pltpu.VMEM((2, cols, 2 * rank), BF16),
            pltpu.VMEM((rank, rank), BF16),
            pltpu.VMEM((NZ, rank // NZ, rank), BF16),
            pltpu.VMEM((rank, rank), BF16),
            pltpu.VMEM((2, NY, cols, rank), BF16),
            pltpu.VMEM((2, 2, NY, cols // 2, rank), BF16),
            dma((14,)),
            dma((2,)),
            dma((2,)),
            dma((2,)),
            dma((2, 2, len(PLACES))),
            dma((2,)),
            dma((2,)),
            dma((2,)),
            dma((2,)),
            dma,
            dma,
            dma((2,)),
            dma((2,)),
            dma((2,)),
            dma((2,)),
            dma((2,)),
            dma((2, 2)),
        ],
        compiler_params=pltpu.CompilerParams(
            collective_id=0, has_side_effects=True, vmem_limit_bytes=67043328 - n * cols * 2
        ),
    )(
        leaf_lists,
        owner,
        cluster_lists,
        group_lists,
        rhs,
        guess,
        diag_blocks,
        precond,
        bases,
        leaf_to_middle_transfer,
        mid_transfer,
        leaf_coupling,
        cluster_coupling,
        group_coupling,
    )


def solution(mesh):
    in_specs = (
        P(("top", "mid", "leaf"), None),
        P(("top", "mid", "leaf"), None),
        P(("top", "mid", "leaf"), None, None),
        P(("top", "mid", "leaf"), None, None),
        P(("top", "mid", "leaf"), None, None),
        P(("top", "mid", "leaf"), None, None),
        P(),
        P(("top", "mid", "leaf"), None, None, None),
        P(("top", "mid"), None, None, None),
        P("top", None, None, None),
        P(("top", "mid", "leaf"), None),
        P(("top", "mid"), None),
        P(("top", "mid"), None),
        P("top", None),
    )
    out_specs = P(("top", "mid", "leaf"), None)
    return jax.shard_map(body, mesh=mesh, in_specs=in_specs, out_specs=out_specs, check_vma=False)
```
